32 devices in a mesh: dp: 1 (over z), cp: 32 (over y, x, core).
Axes of the slice: x: 4, y: 4, z: 1, core: 2. Of those that a mesh axis runs over, the one named last changes fastest.
The devices are a block of a 4x4x8 slice.
Arguments:
- queries: bfloat16 [768, 40, 128], P(('dp', 'cp'))
- key_new: bfloat16 [768, 8, 128], P(('dp', 'cp'))
- value_new: bfloat16 [768, 8, 128], P(('dp', 'cp'))
- key_cache: bfloat16 [32768, 8, 128], P(('dp', 'cp'))
- value_cache: bfloat16 [32768, 8, 128], P(('dp', 'cp'))
- prefix_len: int32 [1], P('dp')
Outputs:
- output 1: bfloat16 [768, 40, 128], P(('dp', 'cp'))
- output 2: float32 [768, 40], P(('dp', 'cp'))
All inputs are finite; a program needn't handle non-finite values.
Results may differ from the reference program's by a relative error of at most 0.00908133.
Values are sent between devices in bfloat16 or wider.
A program may use at most 768 MiB of HBM per device.

```python
import math
import jax
import jax.numpy as jnp
from jax import lax

GROUP_SIZE = 32
NEW_DEV = 24
PREFIX_DEV = 1024
Q_HEADS = 40
KV_HEADS = 8
HEAD_DIM = 128
NEW_LEN = GROUP_SIZE * NEW_DEV
P_MAX = GROUP_SIZE * PREFIX_DEV
GROUP_RATIO = Q_HEADS // KV_HEADS


def setup_inputs(seed: int = 0, part: int = 0) -> dict:
    base_key = jax.random.fold_in(jax.random.key(seed), part)
    rand_keys = jax.random.split(base_key, 9)
    shift_scale = GROUP_SIZE ** 0.5
    new_boost = math.log(P_MAX / NEW_LEN) * 2.0 ** 0.5
    direction = jax.random.normal(rand_keys[0], (KV_HEADS, HEAD_DIM), jnp.float32)
    direction = direction / jnp.linalg.norm(direction, axis=-1, keepdims=True)
    q_mean = jnp.repeat(direction, GROUP_RATIO, axis=0) * HEAD_DIM ** 0.5
    q_noise = jax.random.normal(rand_keys[1], (NEW_LEN, Q_HEADS, HEAD_DIM), jnp.float32)
    queries = (q_noise + q_mean[None]) * 0.5 ** 0.5
    key_new = jax.random.normal(rand_keys[2], (NEW_LEN, KV_HEADS, HEAD_DIM), jnp.float32) + new_boost * direction[None]
    new_shift = jax.random.normal(rand_keys[3], (GROUP_SIZE, 1, KV_HEADS, HEAD_DIM), jnp.float32) * shift_scale
    value_new = jax.random.normal(rand_keys[4], (GROUP_SIZE, NEW_DEV, KV_HEADS, HEAD_DIM), jnp.float32) + new_shift
    key_cache = jax.random.normal(rand_keys[5], (P_MAX, KV_HEADS, HEAD_DIM), jnp.float32)
    cache_shift = jax.random.normal(rand_keys[6], (GROUP_SIZE, 1, KV_HEADS, HEAD_DIM), jnp.float32) * shift_scale
    value_cache = jax.random.normal(rand_keys[7], (GROUP_SIZE, PREFIX_DEV, KV_HEADS, HEAD_DIM), jnp.float32) + cache_shift
    prefix_len = jax.random.randint(rand_keys[8], (1,), (3 * P_MAX) // 4, P_MAX + 1, jnp.int32)
    return {
        'queries': queries.astype(jnp.bfloat16),
        'key_new': key_new.astype(jnp.bfloat16),
        'value_new': value_new.reshape(NEW_LEN, KV_HEADS, HEAD_DIM).astype(jnp.bfloat16),
        'key_cache': key_cache.astype(jnp.bfloat16),
        'value_cache': value_cache.reshape(P_MAX, KV_HEADS, HEAD_DIM).astype(jnp.bfloat16),
        'prefix_len': prefix_len,
    }


def reference(queries, key_new, value_new, key_cache, value_cache, prefix_len):
    prefix_end = prefix_len[0]
    key_pos = jnp.arange(P_MAX + NEW_LEN)
    logit_scale = HEAD_DIM ** -0.5

    def one_head(head_idx):
        kv_idx = head_idx // GROUP_RATIO
        keys_all = jnp.concatenate([lax.dynamic_index_in_dim(key_cache, kv_idx, axis=1, keepdims=False), lax.dynamic_index_in_dim(key_new, kv_idx, axis=1, keepdims=False)], axis=0).astype(jnp.float32)
        vals_all = jnp.concatenate([lax.dynamic_index_in_dim(value_cache, kv_idx, axis=1, keepdims=False), lax.dynamic_index_in_dim(value_new, kv_idx, axis=1, keepdims=False)], axis=0).astype(jnp.float32)
        q_head = lax.dynamic_index_in_dim(queries, head_idx, axis=1, keepdims=False).astype(jnp.float32).reshape(GROUP_SIZE, NEW_DEV, HEAD_DIM)

        def one_block(block_args):
            q_rows, row_start = block_args
            scores = jnp.dot(q_rows, keys_all.T) * logit_scale
            q_pos = row_start + jnp.arange(NEW_DEV)
            visible = jnp.where(key_pos[None, :] < P_MAX, key_pos[None, :] < prefix_end, key_pos[None, :] - P_MAX <= q_pos[:, None])
            scores = jnp.where(visible, scores, -jnp.inf)
            row_max = jnp.max(scores, axis=-1)
            exp_scores = jnp.exp(scores - row_max[:, None])
            row_sum = jnp.sum(exp_scores, axis=-1)
            prob_bf = exp_scores.astype(jnp.bfloat16).astype(jnp.float32)
            block_out = jnp.dot(prob_bf, vals_all) / row_sum[:, None]
            return block_out.astype(jnp.bfloat16), row_max + jnp.log(row_sum)

        head_out, head_lse = lax.map(one_block, (q_head, jnp.arange(GROUP_SIZE) * NEW_DEV))
        return head_out.reshape(NEW_LEN, HEAD_DIM), head_lse.reshape(NEW_LEN)

    all_out, all_lse = lax.map(one_head, jnp.arange(Q_HEADS))
    return jnp.transpose(all_out, (1, 0, 2)), jnp.transpose(all_lse)
```

```python
import functools
import math

import jax
import jax.numpy as jnp
from jax import lax
from jax.experimental import pallas as pl
from jax.experimental.pallas import tpu as pltpu
from jax.sharding import PartitionSpec as P

MASK_FILL = -1e30
LOG2E = math.log2(math.e)
LN2 = math.log(2.0)
CHUNK = 256


def solution(mesh):
    groups = mesh.shape['cp']
    tok_spec = P(('dp', 'cp'))

    def kernel(kv_heads, rows, q_ref, k_ref, vt_ref, bias_ref, o_ref, lse_ref, s0, s1, pbuf):
        scale = LOG2E * q_ref.shape[-1] ** -0.5
        keys = k_ref.shape[1]
        cols = 2 * q_ref.shape[2]
        bounds = [(a, min(a + CHUNK, keys)) for a in range(0, keys, CHUNK)]
        tile = pl.program_id(0)
        my_rank = lax.axis_index('cp')

        def scores(h, s_ref):
            q = jnp.concatenate([q_ref[0, h], q_ref[1, h]], axis=0)
            m8 = jnp.full((8, cols), MASK_FILL, jnp.float32)
            yield None
            for a, b in bounds:
                s = lax.dot_general(k_ref[h, a:b, :], q, (((1,), (1,)), ((), ())), preferred_element_type=jnp.float32)
                bias = bias_ref[a:b, :]
                s = s * scale + jnp.concatenate([bias, bias], axis=1)
                if b == keys:
                    n_new = b - a
                    key = my_rank * rows + lax.broadcasted_iota(jnp.int32, (n_new, cols), 0)
                    col = lax.broadcasted_iota(jnp.int32, (n_new, cols), 1)
                    half = (col >= cols // 2).astype(jnp.int32)
                    col = col - half * (cols // 2)
                    tok5 = (2 * tile + half) * rows * 5 + col
                    s = jnp.where(key * 5 <= tok5, s, MASK_FILL)
                s_ref[a:b, :] = s
                m8 = jnp.maximum(m8, jnp.max(s.reshape((b - a) // 8, 8, cols), axis=0))
                yield None
            yield jnp.max(m8, axis=0, keepdims=True)

        def values(h, s_ref, m):
            l8 = jnp.zeros((8, cols), jnp.float32)
            acc = jnp.zeros((vt_ref.shape[1], cols), jnp.float32)
            yield None
            for a, b in bounds:
                p = jnp.exp2(s_ref[a:b, :] - m)
                l8 = l8 + jnp.sum(p.reshape((b - a) // 8, 8, cols), axis=0)
                acc = acc + lax.dot_general(vt_ref[h, :, a:b], p.astype(jnp.bfloat16), (((1,), (0,)), ((), ())), preferred_element_type=jnp.float32)
                yield None
            l = jnp.sum(l8, axis=0, keepdims=True)
            o = (acc / l).astype(jnp.bfloat16)
            half = cols // 2
            o_ref[0, h] = o[:, :half]
            o_ref[1, h] = o[:, half:]
            lse = (m + jnp.log2(l)) * LN2
            lse_ref[0, h:h + 1, :] = lse[:, :half]
            lse_ref[1, h:h + 1, :] = lse[:, half:]
            yield None

        bufs = (s0, s1)
        m = None
        for x in scores(0, bufs[0]):
            m = x
        for h in range(kv_heads):
            ga = values(h, bufs[h % 2], m)
            gb = scores(h + 1, bufs[(h + 1) % 2]) if h + 1 < kv_heads else iter(())
            m2 = None
            done_a = done_b = False
            while not (done_a and done_b):
                try:
                    m2 = next(gb)
                except StopIteration:
                    done_b = True
                try:
                    next(ga)
                except StopIteration:
                    done_a = True
            m = m2

    def local_attend(queries, key_new, value_new, key_cache, value_cache, prefix_len):
        tok, heads, dim = queries.shape
        cache_len, kv_heads = key_cache.shape[:2]
        ratio = heads // kv_heads
        rows = tok * ratio
        rows_pad = 128
        my_rank = lax.axis_index('cp')
        new_pad = -tok % 16
        q = queries.reshape(tok, kv_heads, ratio, dim).transpose(1, 0, 2, 3).reshape(kv_heads, rows, dim)
        q = jnp.pad(q, ((0, 0), (0, rows_pad - rows), (0, 0)))
        q_all = lax.all_gather(q, 'cp')
        k = jnp.concatenate([key_cache, jnp.pad(key_new, ((0, new_pad), (0, 0), (0, 0)))], axis=0).transpose(1, 0, 2)
        vt = jnp.concatenate([value_cache, jnp.pad(value_new, ((0, new_pad), (0, 0), (0, 0)))], axis=0).transpose(1, 2, 0)
        keys = k.shape[1]
        pos = jnp.arange(keys)
        seen = jnp.where(pos < cache_len, my_rank * cache_len + pos < prefix_len[0], pos < cache_len + tok)
        bias = jnp.broadcast_to(jnp.where(seen, 0.0, MASK_FILL).astype(jnp.float32)[:, None], (keys, 128))
        full = lambda a: pl.BlockSpec(a.shape, lambda i: (0,) * a.ndim)
        o_t, lse = pl.pallas_call(
            functools.partial(kernel, kv_heads, tok),
            grid=(groups // 2,),
            in_specs=[pl.BlockSpec((2, kv_heads, rows_pad, dim), lambda i: (i, 0, 0, 0)), full(k), full(vt), full(bias)],
            out_specs=[pl.BlockSpec((2, kv_heads, dim, rows_pad), lambda i: (i, 0, 0, 0)), pl.BlockSpec((2, kv_heads, rows_pad), lambda i: (i, 0, 0))],
            out_shape=[jax.ShapeDtypeStruct((groups, kv_heads, dim, rows_pad), jnp.bfloat16), jax.ShapeDtypeStruct((groups, kv_heads, rows_pad), jnp.float32)],
            scratch_shapes=[pltpu.VMEM((keys, 2 * rows_pad), jnp.float32), pltpu.VMEM((keys, 2 * rows_pad), jnp.float32), pltpu.VMEM((8, 128), jnp.float32)],
            compiler_params=pltpu.CompilerParams(vmem_limit_bytes=60 * 1024 * 1024),
            name='attend',
        )(q_all, k, vt, bias)
        o_all = lax.all_to_all(o_t, 'cp', 0, 0)
        lse_all = lax.all_to_all(lse, 'cp', 0, 0)
        top = jnp.max(lse_all, axis=0)
        w = jnp.exp(lse_all - top)
        w_sum = jnp.sum(w, axis=0)
        out = jnp.sum(o_all.astype(jnp.float32) * w[:, :, None, :], axis=0) / w_sum[:, None, :]
        out = out[:, :, :rows].astype(jnp.bfloat16).reshape(kv_heads, dim, tok, ratio).transpose(2, 0, 3, 1).reshape(tok, heads, dim)
        row_lse = (top + jnp.log(w_sum))[:, :rows].reshape(kv_heads, tok, ratio).transpose(1, 0, 2).reshape(tok, heads)
        return out, row_lse

    return jax.shard_map(local_attend, mesh=mesh, in_specs=(tok_spec, tok_spec, tok_spec, tok_spec, tok_spec, P('dp')), out_specs=(tok_spec, tok_spec), check_vma=False)
```

```python
import functools
import math

import jax
import jax.numpy as jnp
from jax import lax
from jax.experimental import pallas as pl
from jax.experimental.pallas import tpu as pltpu
from jax.sharding import PartitionSpec as P

MASK_FILL = -1e30
LOG2E = math.log2(math.e)
LN2 = math.log(2.0)
QK_CHUNK = 512
PV_CHUNK = 256
ROW_STEP = 16


def gray(p):
    return p + p // 2 - 2 * (p // 3)


def merge(parts):
    top = functools.reduce(jnp.maximum, [lse for _, lse in parts])
    weights = [jnp.exp2(lse - top) for _, lse in parts]
    total = functools.reduce(jnp.add, weights)
    inv = 1.0 / total
    out = functools.reduce(jnp.add, [o.astype(jnp.float32) * (w * inv) for (o, _), w in zip(parts, weights)])
    return out, top + jnp.log2(total)


def attend(side, tok, ratio, cache_len, q_hbm, k_hbm, v_hbm, bias_ref, out_ref, lse_ref,
           s0, s1, qbuf, kbuf, vbuf, obuf, lbuf, d2o, d2l, aro, arl, bo, bl, fo, fl,
           rq, sq, kv_loc, kv_send, kv_recv, d2_recv, ar_recv, a_send, a2_send, b_recv, b_send):
    heads, keys, dim = kbuf.shape[1:]
    half_cols = qbuf.shape[3]
    cols = 2 * half_cols
    n_blocks = side * side
    scale = LOG2E * dim ** -0.5
    me = lax.axis_index('cp')
    core = me % 2
    other = 1 - core
    chip = me // 2
    y, x = chip // side, chip % side
    f = y * other + x * core
    s = x * other + y * core
    f_unit = side * other + core
    s_unit = side * core + other

    def slot(df, ds):
        return ((f + df) % side) * f_unit + ((s + ds) % side) * s_unit

    def device(df, ds, which):
        return {'cp': slot(df, ds) * 2 + which}

    def remote(src, dst, send, recv, dev):
        return pltpu.make_async_remote_copy(src_ref=src, dst_ref=dst, send_sem=send, recv_sem=recv, device_id=dev, device_id_type=pl.DeviceIdType.MESH)

    peers = [device(0, 0, other), device(1, 0, core), device(side - 1, 0, core)]
    for d in range(1, side):
        peers += [device(0, d, core), device(0, d, other), device(d, 0, other)]
    barrier = pltpu.get_barrier_semaphore()
    for dev in peers:
        pl.semaphore_signal(barrier, inc=1, device_id=dev, device_id_type=pl.DeviceIdType.MESH)

    mine = slot(0, 0)
    loads = [pltpu.make_async_copy(q_hbm.at[core], qbuf.at[mine, core], kv_loc.at[0]),
             pltpu.make_async_copy(k_hbm.at[core], kbuf.at[core], kv_loc.at[1]),
             pltpu.make_async_copy(v_hbm.at[core], vbuf.at[core], kv_loc.at[2])]
    for c in loads:
        c.start()
    pl.semaphore_wait(barrier, len(peers))

    swaps = [remote(q_hbm.at[other], qbuf.at[mine, core], kv_send.at[0], rq.at[mine, core], device(0, 0, other)),
             remote(k_hbm.at[other], kbuf.at[core], kv_send.at[1], kv_recv.at[0], device(0, 0, other)),
             remote(v_hbm.at[other], vbuf.at[core], kv_send.at[2], kv_recv.at[1], device(0, 0, other))]
    for c in swaps:
        c.start()

    sends = []

    def piece(df, ds, j, to_df, to_ds):
        where = slot(df, ds)
        c = remote(qbuf.at[where, j], qbuf.at[where, j], sq.at[len(sends)], rq.at[where, j], device(to_df, to_ds, core))
        sends.append(c)
        return c

    def got(df, ds, j):
        where = slot(df, ds)
        remote(qbuf.at[where, j], qbuf.at[where, j], sq.at[0], rq.at[where, j], device(0, 0, core)).wait_recv()

    back = side - 1
    loads[0].wait()
    around = [(1, 0), (back, 0), (0, 1), (0, back)]
    first = [piece(0, 0, core, a, b) for a, b in around]
    for c in first:
        c.start()
    got(0, 0, other)
    second = [piece(0, 0, other, a, b) for a, b in around]
    for c in second:
        c.start()

    def along_s(df):
        return [piece(df, 0, j, 0, d) for j in (0, 1) for d in (1, back)]

    def forward_s(df):
        return [piece(df, back, 0, 0, 1), piece(df, 1, 1, 0, back)]

    def whole(df, ds):
        return [(df, ds, 0), (df, ds, 1)]

    plan = {
        0: (whole(1, 0) + whole(back, 0) + whole(0, 1) + whole(0, back),
            [piece(back, 0, 0, 1, 0), piece(1, 0, 1, back, 0)] + forward_s(0) + along_s(1)),
        1: ([], along_s(back)),
        2: (whole(0, 2) + whole(2, 0), along_s(2)),
        3: (whole(1, 1) + whole(1, back), forward_s(1)),
        4: (whole(2, 1) + whole(2, back), forward_s(2)),
        5: (whole(back, 1) + whole(back, back), forward_s(back)),
        6: (whole(2, 2), []),
        7: (whole(1, 2) + whole(back, 2), []),
    }

    loads[1].wait()
    loads[2].wait()
    swaps[1].wait_recv()
    swaps[2].wait_recv()

    def place(i):
        g, p = i // side, i % side
        df = (g % 2) * 2 + g // 2
        rev = g // 3
        ds = gray(p * (1 - rev) + (side - 1 - p) * rev)
        return df, ds

    bufs = (s0, s1)
    spans = [(a, b) for a, b in ((0, QK_CHUNK), (QK_CHUNK, keys))]

    def scores(i, h, s_ref, found):
        df, ds = place(i)
        where = slot(df, ds)
        q = jnp.concatenate([qbuf[where, 0, h], qbuf[where, 1, h]], axis=0)
        m8 = jnp.full((8, cols), MASK_FILL, jnp.float32)
        for src in (0, 1):
            for a, b in spans:
                sc = lax.dot_general(kbuf[src, h, a:b, :], q, (((1,), (1,)), ((), ())), preferred_element_type=jnp.float32)
                for r in range(a, b, ROW_STEP):
                    bias = bias_ref[src, r:r + ROW_STEP, :]
                    t = sc[r - a:r - a + ROW_STEP] * scale + jnp.concatenate([bias, bias], axis=1)
                    if r >= cache_len:
                        key = (2 * chip + src) * tok + (r - cache_len) + lax.broadcasted_iota(jnp.int32, t.shape, 0)
                        col = lax.broadcasted_iota(jnp.int32, t.shape, 1)
                        row = 2 * where * (tok * ratio) + col + jnp.where(col >= half_cols, tok * ratio - half_cols, 0)
                        t = jnp.where(key * ratio <= row, t, MASK_FILL)
                    s_ref[src * keys + r:src * keys + r + ROW_STEP, :] = t
                    for u in range(0, ROW_STEP, 8):
                        m8 = jnp.maximum(m8, t[u:u + 8])
                    yield
        found.append(jnp.max(m8, axis=0, keepdims=True))

    def values(i, h, s_ref, m):
        l8 = jnp.zeros((8, cols), jnp.float32)
        acc = None
        for src in (0, 1):
            for a in range(0, keys, PV_CHUNK):
                b = min(a + PV_CHUNK, keys)
                ps = []
                for r in range(a, b, ROW_STEP):
                    p = jnp.exp2(s_ref[src * keys + r:src * keys + r + ROW_STEP, :] - m)
                    for u in range(0, ROW_STEP, 8):
                        l8 = l8 + p[u:u + 8]
                    ps.append(p.astype(jnp.bfloat16))
                    yield
                d = lax.dot_general(vbuf[src, h, :, a:b], jnp.concatenate(ps, axis=0), (((1,), (0,)), ((), ())), preferred_element_type=jnp.float32)
                acc = d if acc is None else acc + d
        l = jnp.sum(l8, axis=0, keepdims=True)
        obuf[i, h] = (acc * (1.0 / l)).astype(jnp.bfloat16)
        lbuf[i, h:h + 1, :] = m + jnp.log2(l)
        yield

    def run(*gens):
        live = list(gens)
        while live:
            for g in list(live):
                try:
                    next(g)
                except StopIteration:
                    live.remove(g)

    pair = heads // 2

    def send_far(i, ds):
        return [remote(obuf.at[i, pl.ds(t * pair, pair)], d2o.at[t, ds], a2_send.at[0, t, ds], d2_recv.at[0, t, ds], device(d, 0, core))
                for t, d in ((0, 1), (1, back))] + [
                remote(lbuf.at[i], d2l.at[t, ds], a2_send.at[1, t, ds], d2_recv.at[1, t, ds], device(d, 0, core)) for t, d in ((0, 1), (1, back))]

    def send_near(i, t, ds):
        d = (1, back)[t]
        return [remote(obuf.at[i], aro.at[t, ds], a_send.at[0, t, ds], ar_recv.at[0, t, ds], device(d, 0, core)),
                remote(lbuf.at[i], arl.at[t, ds], a_send.at[1, t, ds], ar_recv.at[1, t, ds], device(d, 0, core))]

    def add_far(i, t, ds):
        for c in send_far(i, ds)[t::2]:
            c.wait_recv()
        for u in range(pair):
            h = t * pair + u
            o, lse = merge([(obuf[i, h], lbuf[i, h:h + 1, :]), (d2o[t, ds, u], d2l[t, ds, h:h + 1, :])])
            obuf[i, h] = o.astype(jnp.bfloat16)
            lbuf[i, h:h + 1, :] = lse

    def send_home(ds, halves):
        return [c for t in halves for c in (
            remote(bo.at[ds, t], fo.at[core, ds], b_send.at[0, t, ds], b_recv.at[0, core, ds], device(0, ds, t)),
            remote(bl.at[ds, t], fl.at[core, ds], b_send.at[1, t, ds], b_recv.at[1, core, ds], device(0, ds, t)))]

    def gather_row(ds):
        for t in (0, 1):
            for c in send_near(0, t, ds):
                c.wait_recv()
        i = gray(ds)
        for h in range(heads):
            o, lse = merge([(obuf[i, h], lbuf[i, h:h + 1, :])] + [(aro[t, ds, h], arl[t, ds, h:h + 1, :]) for t in (0, 1)])
            o = o.astype(jnp.bfloat16)
            for t in (0, 1):
                bo[ds, t, h] = o[:, t * half_cols:(t + 1) * half_cols]
                bl[ds, t, h:h + 1, :] = lse[:, t * half_cols:(t + 1) * half_cols]

    found = []
    run(scores(0, 0, s0, found))

    def body(i, m):
        for at, (waits, starts) in plan.items():
            @pl.when(i == at)
            def _():
                for w in waits:
                    got(*w)
                for c in starts:
                    c.start()
        nxt = i + 1 - (i + 1) // n_blocks
        for h in range(heads):
            found = []
            last = h + 1 == heads
            run(values(i, h, bufs[h % 2], m), scores(nxt if last else i, 0 if last else h + 1, bufs[(h + 1) % 2], found))
            m = found[0]
        df, ds = place(i)
        g = i // side

        @pl.when(g == 1)
        def _():
            for c in send_far(i, ds):
                c.start()

        @pl.when(g == 2)
        def _():
            add_far(i, 0, ds)
            for c in send_near(i, 0, ds):
                c.start()

        @pl.when(g == 3)
        def _():
            add_far(i, 1, ds)
            for c in send_near(i, 1, ds):
                c.start()

        @pl.when(i >= n_blocks - side + 1)
        def _():
            ds = gray(n_blocks - i)
            gather_row(ds)
            for c in send_home(ds, (0, 1)):
                c.start()
        return m

    lax.fori_loop(0, n_blocks, body, found[0])
    gather_row(0)
    to_sibling = [remote(bo.at[0, other], fo.at[core, 0], b_send.at[0, 0, 0], b_recv.at[0, core, 0], device(0, 0, other)),
                  remote(bl.at[0, other], fl.at[core, 0], b_send.at[1, 0, 0], b_recv.at[1, core, 0], device(0, 0, other))]
    for c in to_sibling:
        c.start()
    fo[core, 0] = bo[0, core]
    fl[core, 0] = bl[0, core]

    for ds in range(1, side):
        for k in (0, 1):
            remote(bo.at[ds, k], fo.at[k, ds], b_send.at[0, 0, 0], b_recv.at[0, k, ds], device(0, 0, core)).wait_recv()
            remote(bl.at[ds, k], fl.at[k, ds], b_send.at[0, 0, 0], b_recv.at[1, k, ds], device(0, 0, core)).wait_recv()
    remote(bo.at[0, 0], fo.at[other, 0], b_send.at[0, 0, 0], b_recv.at[0, other, 0], device(0, 0, core)).wait_recv()
    remote(bl.at[0, 0], fl.at[other, 0], b_send.at[0, 0, 0], b_recv.at[1, other, 0], device(0, 0, core)).wait_recv()
    for k in (0, 1):
        for h in range(heads):
            o, lse = merge([(fo[k, d, h], fl[k, d, h:h + 1, :]) for d in range(side)])
            out_ref[k, h] = o.T.astype(jnp.bfloat16)
            lse_ref[k, h:h + 1, :] = lse * LN2

    for c in swaps + sends + to_sibling:
        c.wait_send()
    for ds in range(side):
        for c in send_far(0, ds) + send_near(0, 0, ds) + send_near(0, 1, ds):
            c.wait_send()
    for ds in range(1, side):
        for c in send_home(ds, (0, 1)):
            c.wait_send()


def solution(mesh):
    groups = mesh.shape['cp']
    side = math.isqrt(groups // 2)
    tok_spec = P(('dp', 'cp'))

    def local_attend(queries, key_new, value_new, key_cache, value_cache, prefix_len):
        tok, heads, dim = queries.shape
        cache_len, kv_heads = key_cache.shape[:2]
        ratio = heads // kv_heads
        half = kv_heads // 2
        rows = tok * ratio
        rows_pad = rows + -rows % 128
        new_pad = -tok % 16
        keys = cache_len + tok + new_pad
        chip = lax.axis_index('cp') // 2
        q = queries.reshape(tok, kv_heads, ratio, dim).transpose(1, 0, 2, 3).reshape(kv_heads, rows, dim)
        q = jnp.pad(q, ((0, 0), (0, rows_pad - rows), (0, 0))).reshape(2, half, rows_pad, dim)
        k = jnp.concatenate([key_cache, jnp.pad(key_new, ((0, new_pad), (0, 0), (0, 0)))], axis=0).transpose(1, 0, 2).reshape(2, half, keys, dim)
        vt = jnp.concatenate([value_cache, jnp.pad(value_new, ((0, new_pad), (0, 0), (0, 0)))], axis=0).transpose(1, 2, 0).reshape(2, half, dim, keys)
        pos = jnp.arange(keys)[None, :]
        start = (chip * 2 + jnp.arange(2)[:, None]) * cache_len
        seen = jnp.where(pos < cache_len, start + pos < prefix_len[0], pos < cache_len + tok)
        bias = jnp.broadcast_to(jnp.where(seen, 0.0, MASK_FILL).astype(jnp.float32)[:, :, None], (2, keys, 128))
        n_blocks = side * side
        bf, f32 = jnp.bfloat16, jnp.float32
        cols = 2 * rows_pad
        dma = pltpu.SemaphoreType.DMA
        out, lse = pl.pallas_call(
            functools.partial(attend, side, tok, ratio, cache_len),
            in_specs=[pl.BlockSpec(memory_space=pl.ANY)] * 3 + [pl.BlockSpec(memory_space=pltpu.VMEM)],
            out_specs=[pl.BlockSpec(memory_space=pltpu.VMEM)] * 2,
            out_shape=[jax.ShapeDtypeStruct((2, half, rows_pad, dim), bf), jax.ShapeDtypeStruct((2, half, rows_pad), f32)],
            scratch_shapes=[
                pltpu.VMEM((2 * keys, cols), f32), pltpu.VMEM((2 * keys, cols), f32),
                pltpu.VMEM((n_blocks, 2, half, rows_pad, dim), bf),
                pltpu.VMEM((2, half, keys, dim), bf), pltpu.VMEM((2, half, dim, keys), bf),
                pltpu.VMEM((n_blocks, half, dim, cols), bf), pltpu.VMEM((n_blocks, half, cols), f32),
                pltpu.VMEM((2, side, half // 2, dim, cols), bf), pltpu.VMEM((2, side, half, cols), f32),
                pltpu.VMEM((2, side, half, dim, cols), bf), pltpu.VMEM((2, side, half, cols), f32),
                pltpu.VMEM((side, 2, half, dim, rows_pad), bf), pltpu.VMEM((side, 2, half, rows_pad), f32),
                pltpu.VMEM((2, side, half, dim, rows_pad), bf), pltpu.VMEM((2, side, half, rows_pad), f32),
                dma((n_blocks, 2)), dma((40,)), dma((3,)), dma((3,)), dma((2,)),
                dma((2, 2, side)), dma((2, 2, side)), dma((2, 2, side)), dma((2, 2, side)), dma((2, 2, side)), dma((2, 2, side)),
            ],
            compiler_params=pltpu.CompilerParams(collective_id=0, has_side_effects=True, vmem_limit_bytes=60 * 1024 * 1024),
            name='attend',
        )(q, k, vt, bias)
        out = out.reshape(kv_heads, rows_pad, dim)[:, :rows].reshape(kv_heads, tok, ratio, dim).transpose(1, 0, 2, 3).reshape(tok, heads, dim)
        lse = lse.reshape(kv_heads, rows_pad)[:, :rows].reshape(kv_heads, tok, ratio).transpose(1, 0, 2).reshape(tok, heads)
        return out, lse

    return jax.shard_map(local_attend, mesh=mesh, in_specs=(tok_spec, tok_spec, tok_spec, tok_spec, tok_spec, P('dp')), out_specs=(tok_spec, tok_spec), check_vma=False)
```

```python
import functools
import math

import jax
import jax.numpy as jnp
from jax import lax
from jax.experimental import pallas as pl
from jax.experimental.pallas import tpu as pltpu
from jax.sharding import PartitionSpec as P

MASK_FILL = -1e30
LOG2E = math.log2(math.e)
LN2 = math.log(2.0)
QK_CHUNK = 512
PV_CHUNK = 256
ROW_STEP = 16


def gray(p):
    return p + p // 2 - 2 * (p // 3)


def merge(parts):
    top = functools.reduce(jnp.maximum, [lse for _, lse in parts])
    weights = [jnp.exp2(lse - top) for _, lse in parts]
    total = functools.reduce(jnp.add, weights)
    inv = 1.0 / total
    out = functools.reduce(jnp.add, [o.astype(jnp.float32) * (w * inv) for (o, _), w in zip(parts, weights)])
    return out, top + jnp.log2(total)


def attend(side, tok, ratio, cache_len, prefix_ref, q_hbm, kn_hbm, vn_hbm, k_hbm, v_hbm, out_ref, lse_ref,
           qraw, knraw, vnraw, kraw, vraw, stage, qst, ostage, lstage, bias_ref, s0, s1, qbuf, kbuf, vbuf, obuf, lbuf, d2o, d2l, aro, arl, bo, bl, fo, fl,
           loads, rq, sq, kv_loc, kv_send, kv_recv, q_swap, d2_recv, ar_recv, a_send, a2_send, b_recv, b_send):
    heads, keys, dim = kbuf.shape[1:]
    half_cols = qbuf.shape[3]
    cols = 2 * half_cols
    n_blocks = side * side
    scale = LOG2E * dim ** -0.5
    me = lax.axis_index('cp')
    core = me % 2
    other = 1 - core
    chip = me // 2
    y, x = chip // side, chip % side
    f = y * other + x * core
    s = x * other + y * core
    f_unit = side * other + core
    s_unit = side * core + other

    def slot(df, ds):
        return ((f + df) % side) * f_unit + ((s + ds) % side) * s_unit

    def device(df, ds, which):
        return {'cp': slot(df, ds) * 2 + which}

    def remote(src, dst, send, recv, dev):
        return pltpu.make_async_remote_copy(src_ref=src, dst_ref=dst, send_sem=send, recv_sem=recv, device_id=dev, device_id_type=pl.DeviceIdType.MESH)

    peers = [device(0, 0, other), device(1, 0, core), device(side - 1, 0, core)]
    for d in range(1, side):
        peers += [device(0, d, core), device(0, d, other), device(d, 0, other)]
    barrier = pltpu.get_barrier_semaphore()
    for dev in peers:
        pl.semaphore_signal(barrier, inc=1, device_id=dev, device_id_type=pl.DeviceIdType.MESH)

    mine = slot(0, 0)
    kv_heads = 2 * heads
    chunk = stage.shape[1] // kv_heads
    n_chunks = cache_len // chunk
    small = [pltpu.make_async_copy(src, dst, loads.at[n, 0]) for n, (src, dst) in enumerate(((q_hbm, qraw), (kn_hbm, knraw), (vn_hbm, vnraw)))]

    def raw_copy(n, c):
        rows = pl.ds(pl.multiple_of(c * chunk * kv_heads, chunk * kv_heads), chunk * kv_heads)
        src, dst = ((k_hbm, kraw), (v_hbm, vraw))[n]
        return pltpu.make_async_copy(src.at[rows], dst.at[rows], loads.at[3 + n, c])

    for c in small:
        c.start()
    for c in range(n_chunks):
        for n in (0, 1):
            raw_copy(n, c).start()

    for n, holder in enumerate((core, other)):
        pos = lax.broadcasted_iota(jnp.int32, (cache_len, 128), 0) + (2 * chip + holder) * cache_len
        bias_ref[n, :cache_len] = jnp.where(pos < prefix_ref[0], 0.0, MASK_FILL)
        bias_ref[n, cache_len:] = jnp.where(lax.broadcasted_iota(jnp.int32, (keys - cache_len, 128), 0) < tok, 0.0, MASK_FILL)

    small[0].wait()
    ostage[...] = qraw[...].astype(jnp.float32)
    for h in range(kv_heads):
        rows = [ostage[pl.ds(h * ratio + g, tok, stride=kv_heads * ratio), :] for g in range(ratio)]
        rows.append(jnp.zeros((half_cols - tok * ratio, dim), jnp.float32))
        qst[h // heads, h % heads] = jnp.concatenate(rows, axis=0).astype(jnp.bfloat16)

    small[1].wait()
    small[2].wait()
    stage[0, :tok * kv_heads] = knraw[...].astype(jnp.float32)
    stage[1, :tok * kv_heads] = vnraw[...].astype(jnp.float32)
    blank = jnp.zeros((keys - cache_len - tok, dim), jnp.float32)
    for h in range(kv_heads):
        new_k = jnp.concatenate([stage[0, pl.ds(h, tok, stride=kv_heads), :], blank], axis=0)
        new_v = jnp.concatenate([stage[1, pl.ds(h, tok, stride=kv_heads), :], blank], axis=0)
        kbuf[h // heads, h % heads, cache_len:] = new_k.astype(jnp.bfloat16)
        vbuf[h // heads, h % heads, :, cache_len:] = new_v.T.astype(jnp.bfloat16)

    pl.semaphore_wait(barrier, len(peers))
    local_q = pltpu.make_async_copy(qst.at[core], qbuf.at[mine, core], kv_loc.at[0])
    local_q.start()
    swap_q = remote(qst.at[other], qbuf.at[mine, core], q_swap, rq.at[mine, core], device(0, 0, other))
    swap_q.start()

    def swap(c):
        n_rows = chunk if isinstance(c, int) is False or c < n_chunks else keys - cache_len
        at = pl.ds(c * chunk if isinstance(c, int) else pl.multiple_of(c * chunk, chunk), n_rows)
        return [remote(kbuf.at[other, :, at, :], kbuf.at[2, :, at, :], kv_send.at[0, c], kv_recv.at[0, c], device(0, 0, other)),
                remote(vbuf.at[other, :, :, at], vbuf.at[2, :, :, at], kv_send.at[1, c], kv_recv.at[1, c], device(0, 0, other))]

    sends = []

    def piece(df, ds, j, to_df, to_ds):
        where = slot(df, ds)
        c = remote(qbuf.at[where, j], qbuf.at[where, j], sq.at[len(sends)], rq.at[where, j], device(to_df, to_ds, core))
        sends.append(c)
        return c

    def got(df, ds, j):
        where = slot(df, ds)
        remote(qbuf.at[where, j], qbuf.at[where, j], sq.at[0], rq.at[where, j], device(0, 0, core)).wait_recv()

    back = side - 1
    local_q.wait()
    around = [(1, 0), (back, 0), (0, 1), (0, back)]
    first = [piece(0, 0, core, a, b) for a, b in around]
    for c in first:
        c.start()
    second = [piece(0, 0, other, a, b) for a, b in around]

    def relayout(c, carry):
        @pl.when(c == 1)
        def _():
            got(0, 0, other)
            for d in second:
                d.start()

        @pl.when(c > 0)
        def _():
            for d in swap(c - 1):
                d.start()

        rows = pl.ds(pl.multiple_of(c * chunk * kv_heads, chunk * kv_heads), chunk * kv_heads)
        at = pl.ds(pl.multiple_of(c * chunk, chunk), chunk)
        raw_copy(0, c).wait()
        raw_copy(1, c).wait()
        stage[0] = kraw[rows, :].astype(jnp.float32)
        stage[1] = vraw[rows, :].astype(jnp.float32)
        for h in range(kv_heads):
            kbuf[h // heads, h % heads, at, :] = stage[0, pl.ds(h, chunk, stride=kv_heads), :].astype(jnp.bfloat16)
            vbuf[h // heads, h % heads, :, at] = stage[1, pl.ds(h, chunk, stride=kv_heads), :].T.astype(jnp.bfloat16)
        return carry

    lax.fori_loop(0, n_chunks, relayout, 0)
    swaps = [d for c in range(n_chunks + 1) for d in swap(c)]
    for d in swaps[2 * n_chunks - 2:]:
        d.start()

    def along_s(df):
        return [piece(df, 0, j, 0, d) for j in (0, 1) for d in (1, back)]

    def forward_s(df):
        return [piece(df, back, 0, 0, 1), piece(df, 1, 1, 0, back)]

    def whole(df, ds):
        return [(df, ds, 0), (df, ds, 1)]

    plan = {
        0: (whole(1, 0) + whole(back, 0) + whole(0, 1) + whole(0, back),
            [piece(back, 0, 0, 1, 0), piece(1, 0, 1, back, 0)] + forward_s(0) + along_s(1)),
        1: ([], along_s(back)),
        2: (whole(0, 2) + whole(2, 0), along_s(2)),
        3: (whole(1, 1) + whole(1, back), forward_s(1)),
        4: (whole(2, 1) + whole(2, back), forward_s(2)),
        5: (whole(back, 1) + whole(back, back), forward_s(back)),
        6: (whole(2, 2), []),
        7: (whole(1, 2) + whole(back, 2), []),
    }

    for d in swaps:
        d.wait_recv()

    col = lax.broadcasted_iota(jnp.int32, (1, cols), 1)
    row = col - jnp.where(col >= half_cols, half_cols, 0)
    for g in range(ratio):
        row = row - jnp.where(row >= tok, tok, 0)
    q_tok = row + jnp.where(col >= half_cols, tok, 0)

    def place(i):
        g, p = i // side, i % side
        df = (g % 2) * 2 + g // 2
        rev = g // 3
        ds = gray(p * (1 - rev) + (side - 1 - p) * rev)
        return df, ds

    bufs = (s0, s1)
    spans = [(a, b) for a, b in ((0, QK_CHUNK), (QK_CHUNK, keys))]

    def scores(i, h, s_ref, found):
        df, ds = place(i)
        where = slot(df, ds)
        q = jnp.concatenate([qbuf[where, 0, h], qbuf[where, 1, h]], axis=0)
        m8 = jnp.full((8, cols), MASK_FILL, jnp.float32)
        for src, (held, holder) in enumerate(((core, core), (2, other))):
            for a, b in spans:
                sc = lax.dot_general(kbuf[held, h, a:b, :], q, (((1,), (1,)), ((), ())), preferred_element_type=jnp.float32)
                for r in range(a, b, ROW_STEP):
                    bias = bias_ref[src, r:r + ROW_STEP, :]
                    t = sc[r - a:r - a + ROW_STEP] * scale + jnp.concatenate([bias, bias], axis=1)
                    if r >= cache_len:
                        first_key = (2 * chip + holder) * tok + (r - cache_len) - 2 * where * tok
                        t = jnp.where(first_key + lax.broadcasted_iota(jnp.int32, t.shape, 0) <= q_tok, t, MASK_FILL)
                    s_ref[src * keys + r:src * keys + r + ROW_STEP, :] = t
                    for u in range(0, ROW_STEP, 8):
                        m8 = jnp.maximum(m8, t[u:u + 8])
                    yield
        found.append(jnp.max(m8, axis=0, keepdims=True))

    def values(i, h, s_ref, m):
        l8 = jnp.zeros((8, cols), jnp.float32)
        acc = None
        for src, held in enumerate((core, 2)):
            for a in range(0, keys, PV_CHUNK):
                b = min(a + PV_CHUNK, keys)
                ps = []
                for r in range(a, b, ROW_STEP):
                    p = jnp.exp2(s_ref[src * keys + r:src * keys + r + ROW_STEP, :] - m)
                    for u in range(0, ROW_STEP, 8):
                        l8 = l8 + p[u:u + 8]
                    ps.append(p.astype(jnp.bfloat16))
                    yield
                d = lax.dot_general(vbuf[held, h, :, a:b], jnp.concatenate(ps, axis=0), (((1,), (0,)), ((), ())), preferred_element_type=jnp.float32)
                acc = d if acc is None else acc + d
        l = jnp.sum(l8, axis=0, keepdims=True)
        obuf[i, h] = (acc * (1.0 / l)).astype(jnp.bfloat16)
        lbuf[i, h:h + 1, :] = m + jnp.log2(l)
        yield

    def run(*gens):
        live = list(gens)
        while live:
            for g in list(live):
                try:
                    next(g)
                except StopIteration:
                    live.remove(g)

    pair = heads // 2

    def send_far(i, ds):
        return [remote(obuf.at[i, pl.ds(t * pair, pair)], d2o.at[t, ds], a2_send.at[0, t, ds], d2_recv.at[0, t, ds], device(d, 0, core))
                for t, d in ((0, 1), (1, back))] + [
                remote(lbuf.at[i], d2l.at[t, ds], a2_send.at[1, t, ds], d2_recv.at[1, t, ds], device(d, 0, core)) for t, d in ((0, 1), (1, back))]

    def send_near(i, t, ds):
        d = (1, back)[t]
        return [remote(obuf.at[i], aro.at[t, ds], a_send.at[0, t, ds], ar_recv.at[0, t, ds], device(d, 0, core)),
                remote(lbuf.at[i], arl.at[t, ds], a_send.at[1, t, ds], ar_recv.at[1, t, ds], device(d, 0, core))]

    def add_far(i, t, ds):
        for c in send_far(i, ds)[t::2]:
            c.wait_recv()
        for u in range(pair):
            h = t * pair + u
            o, lse = merge([(obuf[i, h], lbuf[i, h:h + 1, :]), (d2o[t, ds, u], d2l[t, ds, h:h + 1, :])])
            obuf[i, h] = o.astype(jnp.bfloat16)
            lbuf[i, h:h + 1, :] = lse

    def send_home(ds, halves):
        return [c for t in halves for c in (
            remote(bo.at[ds, t], fo.at[core, ds], b_send.at[0, t, ds], b_recv.at[0, core, ds], device(0, ds, t)),
            remote(bl.at[ds, t], fl.at[core, ds], b_send.at[1, t, ds], b_recv.at[1, core, ds], device(0, ds, t)))]

    def gather_row(ds):
        for t in (0, 1):
            for c in send_near(0, t, ds):
                c.wait_recv()
        i = gray(ds)
        for h in range(heads):
            o, lse = merge([(obuf[i, h], lbuf[i, h:h + 1, :])] + [(aro[t, ds, h], arl[t, ds, h:h + 1, :]) for t in (0, 1)])
            o = o.astype(jnp.bfloat16)
            for t in (0, 1):
                bo[ds, t, h] = o[:, t * half_cols:(t + 1) * half_cols]
                bl[ds, t, h:h + 1, :] = lse[:, t * half_cols:(t + 1) * half_cols]

    found = []
    run(scores(0, 0, s0, found))

    def body(i, m):
        for at, (waits, starts) in plan.items():
            @pl.when(i == at)
            def _():
                for w in waits:
                    got(*w)
                for c in starts:
                    c.start()
        nxt = i + 1 - (i + 1) // n_blocks
        for h in range(heads):
            found = []
            last = h + 1 == heads
            run(values(i, h, bufs[h % 2], m), scores(nxt if last else i, 0 if last else h + 1, bufs[(h + 1) % 2], found))
            m = found[0]
        df, ds = place(i)
        g = i // side

        @pl.when(g == 1)
        def _():
            for c in send_far(i, ds):
                c.start()

        @pl.when(g == 2)
        def _():
            add_far(i, 0, ds)
            for c in send_near(i, 0, ds):
                c.start()

        @pl.when(g == 3)
        def _():
            add_far(i, 1, ds)
            for c in send_near(i, 1, ds):
                c.start()

        @pl.when(i >= n_blocks - side + 1)
        def _():
            ds = gray(n_blocks - i)
            gather_row(ds)
            for c in send_home(ds, (0, 1)):
                c.start()
        return m

    lax.fori_loop(0, n_blocks, body, found[0])
    gather_row(0)
    to_sibling = [remote(bo.at[0, other], fo.at[core, 0], b_send.at[0, 0, 0], b_recv.at[0, core, 0], device(0, 0, other)),
                  remote(bl.at[0, other], fl.at[core, 0], b_send.at[1, 0, 0], b_recv.at[1, core, 0], device(0, 0, other))]
    for c in to_sibling:
        c.start()
    fo[core, 0] = bo[0, core]
    fl[core, 0] = bl[0, core]

    for ds in range(1, side):
        for k in (0, 1):
            remote(bo.at[ds, k], fo.at[k, ds], b_send.at[0, 0, 0], b_recv.at[0, k, ds], device(0, 0, core)).wait_recv()
            remote(bl.at[ds, k], fl.at[k, ds], b_send.at[0, 0, 0], b_recv.at[1, k, ds], device(0, 0, core)).wait_recv()
    remote(bo.at[0, 0], fo.at[other, 0], b_send.at[0, 0, 0], b_recv.at[0, other, 0], device(0, 0, core)).wait_recv()
    remote(bl.at[0, 0], fl.at[other, 0], b_send.at[0, 0, 0], b_recv.at[1, other, 0], device(0, 0, core)).wait_recv()
    for k in (0, 1):
        for h in range(heads):
            o, lse = merge([(fo[k, d, h], fl[k, d, h:h + 1, :]) for d in range(side)])
            o = o.T
            for g in range(ratio):
                ostage[pl.ds((k * heads + h) * ratio + g, tok, stride=kv_heads * ratio), :] = o[g * tok:(g + 1) * tok]
            lstage[k * heads + h:k * heads + h + 1, :] = lse * LN2
    out_ref[...] = ostage[...].astype(jnp.bfloat16)
    lse = lstage[:kv_heads, :]
    for g in range(ratio):
        lstage[pl.ds(kv_heads + g, kv_heads, stride=ratio), :] = lse if g == 0 else pltpu.roll(lse, half_cols - g * tok, 1)
    lse_ref[...] = lstage[kv_heads:kv_heads * (ratio + 1), :].T[:tok]

    for c in swaps + sends + to_sibling + [swap_q]:
        c.wait_send()
    for ds in range(side):
        for c in send_far(0, ds) + send_near(0, 0, ds) + send_near(0, 1, ds):
            c.wait_send()
    for ds in range(1, side):
        for c in send_home(ds, (0, 1)):
            c.wait_send()


def solution(mesh):
    groups = mesh.shape['cp']
    side = math.isqrt(groups // 2)
    tok_spec = P(('dp', 'cp'))

    def local_attend(queries, key_new, value_new, key_cache, value_cache, prefix_len):
        tok, heads, dim = queries.shape
        cache_len, kv_heads = key_cache.shape[:2]
        ratio = heads // kv_heads
        half = kv_heads // 2
        rows = tok * ratio
        rows_pad = rows + -rows % 128
        new_pad = -tok % 16
        keys = cache_len + tok + new_pad
        chunk = cache_len // 4
        n_blocks = side * side
        bf, f32 = jnp.bfloat16, jnp.float32
        cols = 2 * rows_pad
        dma = pltpu.SemaphoreType.DMA
        out, lse = pl.pallas_call(
            functools.partial(attend, side, tok, ratio, cache_len),
            in_specs=[pl.BlockSpec(memory_space=pltpu.SMEM)] + [pl.BlockSpec(memory_space=pl.ANY)] * 5,
            out_specs=[pl.BlockSpec(memory_space=pltpu.VMEM)] * 2,
            out_shape=[jax.ShapeDtypeStruct((tok * heads, dim), bf), jax.ShapeDtypeStruct((tok, heads), f32)],
            scratch_shapes=[
                pltpu.VMEM((tok * heads, dim), bf), pltpu.VMEM((tok * kv_heads, dim), bf), pltpu.VMEM((tok * kv_heads, dim), bf),
                pltpu.VMEM((cache_len * kv_heads, dim), bf), pltpu.VMEM((cache_len * kv_heads, dim), bf),
                pltpu.VMEM((2, chunk * kv_heads, dim), f32), pltpu.VMEM((2, half, rows_pad, dim), bf),
                pltpu.VMEM((tok * heads, dim), f32), pltpu.VMEM((kv_heads * (ratio + 1), rows_pad), f32),
                pltpu.VMEM((2, keys, 128), f32),
                pltpu.VMEM((2 * keys, cols), f32), pltpu.VMEM((2 * keys, cols), f32),
                pltpu.VMEM((n_blocks, 2, half, rows_pad, dim), bf),
                pltpu.VMEM((3, half, keys, dim), bf), pltpu.VMEM((3, half, dim, keys), bf),
                pltpu.VMEM((n_blocks, half, dim, cols), bf), pltpu.VMEM((n_blocks, half, cols), f32),
                pltpu.VMEM((2, side, half // 2, dim, cols), bf), pltpu.VMEM((2, side, half, cols), f32),
                pltpu.VMEM((2, side, half, dim, cols), bf), pltpu.VMEM((2, side, half, cols), f32),
                pltpu.VMEM((side, 2, half, dim, rows_pad), bf), pltpu.VMEM((side, 2, half, rows_pad), f32),
                pltpu.VMEM((2, side, half, dim, rows_pad), bf), pltpu.VMEM((2, side, half, rows_pad), f32),
                dma((5, 4)), dma((n_blocks, 2)), dma((40,)), dma((3,)), dma((2, 5)), dma((2, 5)), dma,
                dma((2, 2, side)), dma((2, 2, side)), dma((2, 2, side)), dma((2, 2, side)), dma((2, 2, side)), dma((2, 2, side)),
            ],
            compiler_params=pltpu.CompilerParams(collective_id=0, has_side_effects=True, vmem_limit_bytes=60 * 1024 * 1024),
            name='attend',
        )(prefix_len, *[a.reshape(-1, dim) for a in (queries, key_new, value_new, key_cache, value_cache)])
        return out.reshape(tok, heads, dim), lse

    return jax.shard_map(local_attend, mesh=mesh, in_specs=(tok_spec, tok_spec, tok_spec, tok_spec, tok_spec, P('dp')), out_specs=(tok_spec, tok_spec), check_vma=False)
```

```python
import functools
import math

import jax
import jax.numpy as jnp
from jax import lax
from jax.experimental import pallas as pl
from jax.experimental.pallas import tpu as pltpu
from jax.sharding import PartitionSpec as P

MASK_FILL = -1e30
LOG2E = math.log2(math.e)
LN2 = math.log(2.0)
QK_CHUNK = 512
PV_CHUNK = 256
ROW_STEP = 16


def gray(p):
    return p + p // 2 - 2 * (p // 3)


def merge(parts):
    top = functools.reduce(jnp.maximum, [lse for _, lse in parts])
    weights = [jnp.exp2(lse - top) for _, lse in parts]
    total = functools.reduce(jnp.add, weights)
    inv = 1.0 / total
    out = functools.reduce(jnp.add, [o.astype(jnp.float32) * (w * inv) for (o, _), w in zip(parts, weights)])
    return out, top + jnp.log2(total)


def attend(side, tok, ratio, cache_len, prefix_ref, q_hbm, kn_hbm, vn_hbm, k_hbm, v_hbm, out_ref, lse_ref,
           qraw, knraw, vnraw, kraw, vraw, stage, qst, ostage, lstage, bias_ref, s0, s1, qbuf, kbuf, vbuf, kx, vx, kcat, vcat, obuf, lbuf, d2o, d2l, aro, arl, bo, bl, fo, fl,
           loads, rq, sq, kv_loc, kv_send, kv_recv, q_swap, d2_recv, ar_recv, a_send, a2_send, b_recv, b_send):
    heads, dim = kbuf.shape[1], kbuf.shape[3]
    n_new = kx.shape[2]
    half_cols = qbuf.shape[3]
    cols = 2 * half_cols
    n_blocks = side * side
    scale = LOG2E * dim ** -0.5
    me = lax.axis_index('cp')
    core = me % 2
    other = 1 - core
    chip = me // 2
    y, x = chip // side, chip % side
    f = y * other + x * core
    s = x * other + y * core
    f_unit = side * other + core
    s_unit = side * core + other

    def slot(df, ds):
        return ((f + df) % side) * f_unit + ((s + ds) % side) * s_unit

    def device(df, ds, which):
        return {'cp': slot(df, ds) * 2 + which}

    def remote(src, dst, send, recv, dev):
        return pltpu.make_async_remote_copy(src_ref=src, dst_ref=dst, send_sem=send, recv_sem=recv, device_id=dev, device_id_type=pl.DeviceIdType.MESH)

    peers = [device(0, 0, other), device(1, 0, core), device(side - 1, 0, core)]
    for d in range(1, side):
        peers += [device(0, d, core), device(0, d, other), device(d, 0, other)]
    barrier = pltpu.get_barrier_semaphore()
    for dev in peers:
        pl.semaphore_signal(barrier, inc=1, device_id=dev, device_id_type=pl.DeviceIdType.MESH)

    mine = slot(0, 0)
    kv_heads = 2 * heads
    chunk = stage.shape[1] // kv_heads
    n_chunks = cache_len // chunk
    small = [pltpu.make_async_copy(src, dst, loads.at[n, 0]) for n, (src, dst) in enumerate(((q_hbm, qraw), (kn_hbm, knraw), (vn_hbm, vnraw)))]

    def raw_copy(n, c):
        rows = pl.ds(pl.multiple_of(c * chunk * kv_heads, chunk * kv_heads), chunk * kv_heads)
        src, dst = ((k_hbm, kraw), (v_hbm, vraw))[n]
        return pltpu.make_async_copy(src.at[rows], dst.at[rows], loads.at[3 + n, c])

    for c in small:
        c.start()
    for c in range(n_chunks):
        for n in (0, 1):
            raw_copy(n, c).start()

    for n, holder in enumerate((core, other)):
        pos = lax.broadcasted_iota(jnp.int32, (cache_len, 128), 0) + (2 * chip + holder) * cache_len
        bias_ref[n] = jnp.where(pos < prefix_ref[0], 0.0, MASK_FILL)

    small[0].wait()
    ostage[...] = qraw[...].astype(jnp.float32)
    for h in range(kv_heads):
        rows = [ostage[pl.ds(h * ratio + g, tok, stride=kv_heads * ratio), :] for g in range(ratio)]
        rows.append(jnp.zeros((half_cols - tok * ratio, dim), jnp.float32))
        qst[h // heads, h % heads] = jnp.concatenate(rows, axis=0).astype(jnp.bfloat16)

    small[1].wait()
    small[2].wait()
    stage[0, :tok * kv_heads] = knraw[...].astype(jnp.float32)
    stage[1, :tok * kv_heads] = vnraw[...].astype(jnp.float32)
    blank = jnp.zeros((n_new - tok, dim), jnp.float32)
    for h in range(kv_heads):
        new_k = jnp.concatenate([stage[0, pl.ds(h, tok, stride=kv_heads), :], blank], axis=0)
        new_v = jnp.concatenate([stage[1, pl.ds(h, tok, stride=kv_heads), :], blank], axis=0)
        kx[h // heads, h % heads] = new_k.astype(jnp.bfloat16)
        vx[h // heads, h % heads] = new_v.astype(jnp.bfloat16)

    pl.semaphore_wait(barrier, len(peers))
    local_q = pltpu.make_async_copy(qst.at[core], qbuf.at[mine, core], kv_loc.at[0])
    local_q.start()
    swap_q = remote(qst.at[other], qbuf.at[mine, core], q_swap, rq.at[mine, core], device(0, 0, other))
    swap_q.start()

    swap_new = [remote(b.at[other], b.at[2], kv_send.at[n, n_chunks], kv_recv.at[n, n_chunks], device(0, 0, other)) for n, b in enumerate((kx, vx))]
    for c in swap_new:
        c.start()

    def swap(c):
        at = pl.ds(c * chunk if isinstance(c, int) else pl.multiple_of(c * chunk, chunk), chunk)
        return [remote(kbuf.at[other, :, at, :], kbuf.at[2, :, at, :], kv_send.at[0, c], kv_recv.at[0, c], device(0, 0, other)),
                remote(vbuf.at[other, :, :, at], vbuf.at[2, :, :, at], kv_send.at[1, c], kv_recv.at[1, c], device(0, 0, other))]

    sends = []

    def piece(df, ds, j, to_df, to_ds):
        where = slot(df, ds)
        c = remote(qbuf.at[where, j], qbuf.at[where, j], sq.at[len(sends)], rq.at[where, j], device(to_df, to_ds, core))
        sends.append(c)
        return c

    def got(df, ds, j):
        where = slot(df, ds)
        remote(qbuf.at[where, j], qbuf.at[where, j], sq.at[0], rq.at[where, j], device(0, 0, core)).wait_recv()

    back = side - 1
    local_q.wait()
    around = [(1, 0), (back, 0), (0, 1), (0, back)]
    first = [piece(0, 0, core, a, b) for a, b in around]
    for c in first:
        c.start()
    second = [piece(0, 0, other, a, b) for a, b in around]

    def relayout(c, carry):
        @pl.when(c == 1)
        def _():
            got(0, 0, other)
            for d in second:
                d.start()

        @pl.when(c > 0)
        def _():
            for d in swap(c - 1):
                d.start()

        rows = pl.ds(pl.multiple_of(c * chunk * kv_heads, chunk * kv_heads), chunk * kv_heads)
        at = pl.ds(pl.multiple_of(c * chunk, chunk), chunk)
        raw_copy(0, c).wait()
        raw_copy(1, c).wait()
        stage[0] = kraw[rows, :].astype(jnp.float32)
        stage[1] = vraw[rows, :].astype(jnp.float32)
        for h in range(kv_heads):
            kbuf[h // heads, h % heads, at, :] = stage[0, pl.ds(h, chunk, stride=kv_heads), :].astype(jnp.bfloat16)
            vbuf[h // heads, h % heads, :, at] = stage[1, pl.ds(h, chunk, stride=kv_heads), :].T.astype(jnp.bfloat16)
        return carry

    lax.fori_loop(0, n_chunks, relayout, 0)
    swaps = [d for c in range(n_chunks) for d in swap(c)]
    for d in swaps[-2:]:
        d.start()
    swaps += swap_new

    def along_s(df):
        return [piece(df, 0, j, 0, d) for j in (0, 1) for d in (1, back)]

    def forward_s(df):
        return [piece(df, back, 0, 0, 1), piece(df, 1, 1, 0, back)]

    def whole(df, ds):
        return [(df, ds, 0), (df, ds, 1)]

    early = [piece(back, 0, 0, 1, 0), piece(1, 0, 1, back, 0)]
    plan = {
        0: ([], along_s(1)),
        1: (whole(2, 0), along_s(2)),
        2: (whole(2, 1) + whole(2, back) + whole(1, 1) + whole(1, back), forward_s(1)),
        3: ([], forward_s(2) + along_s(back)),
        4: (whole(2, 2), forward_s(0)),
        5: (whole(back, 1) + whole(back, back), forward_s(back)),
        6: (whole(1, 2), []),
        7: (whole(0, 2), []),
        8: (whole(back, 2), []),
    }
    for w in whole(1, 0) + whole(back, 0) + whole(0, 1) + whole(0, back):
        got(*w)
    for d in early:
        d.start()

    for d in swaps:
        d.wait_recv()

    for h in range(heads):
        kcat[h] = jnp.concatenate([kx[core, h], kx[2, h]], axis=0)
        vcat[h] = jnp.concatenate([vx[core, h], vx[2, h]], axis=0).astype(jnp.float32).T.astype(jnp.bfloat16)

    col = lax.broadcasted_iota(jnp.int32, (1, cols), 1)
    row = col - jnp.where(col >= half_cols, half_cols, 0)
    for g in range(ratio):
        row = row - jnp.where(row >= tok, tok, 0)
    q_tok = row + jnp.where(col >= half_cols, tok, 0)

    def place(i):
        late = (i + 2) // n_blocks
        inner = (i + n_blocks - 2) // n_blocks - late
        g = (i + 2) // side - 1
        df = inner * (2 - g + (g // 2) * 3)
        turn = inner * ((i + 2) % side + g // 2) + (1 - inner) * (i - (n_blocks - side) * late + 1)
        return df, gray(turn % side)

    bufs = (s0, s1)
    tiles = [(n, a) for n in (0, 1) for a in range(0, cache_len, QK_CHUNK)]

    def scores(i, h, s_ref, found):
        df, ds = place(i)
        where = slot(df, ds)
        q = jnp.concatenate([qbuf[where, 0, h], qbuf[where, 1, h]], axis=0)
        m8 = jnp.full((8, cols), MASK_FILL, jnp.float32)
        for n, a in tiles + [(2, 0)]:
            k = kcat[h] if n == 2 else kbuf[(core, 2)[n], h, a:a + QK_CHUNK, :]
            sc = lax.dot_general(k, q, (((1,), (1,)), ((), ())), preferred_element_type=jnp.float32)
            for r in range(0, k.shape[0], ROW_STEP):
                t = sc[r:r + ROW_STEP] * scale
                if n < 2:
                    bias = bias_ref[n, a + r:a + r + ROW_STEP, :]
                    t = t + jnp.concatenate([bias, bias], axis=1)
                else:
                    step = lax.broadcasted_iota(jnp.int32, t.shape, 0) + r % n_new
                    first_key = (2 * chip + (core, other)[r // n_new]) * tok - 2 * where * tok
                    t = jnp.where((first_key + step <= q_tok) & (step < tok), t, MASK_FILL)
                at = n * cache_len + a + r
                s_ref[at:at + ROW_STEP, :] = t
                for u in range(0, ROW_STEP, 8):
                    m8 = jnp.maximum(m8, t[u:u + 8])
                yield
        found.append(jnp.max(m8, axis=0, keepdims=True))

    def values(i, h, s_ref, m):
        l8 = jnp.zeros((8, cols), jnp.float32)
        acc = None
        for n, a in [(n, a) for n in (0, 1) for a in range(0, cache_len, PV_CHUNK)] + [(2, 0)]:
            v = vcat[h] if n == 2 else vbuf[(core, 2)[n], h, :, a:a + PV_CHUNK]
            ps = []
            for r in range(0, v.shape[1], ROW_STEP):
                at = n * cache_len + a + r
                p = jnp.exp2(s_ref[at:at + ROW_STEP, :] - m)
                for u in range(0, ROW_STEP, 8):
                    l8 = l8 + p[u:u + 8]
                ps.append(p.astype(jnp.bfloat16))
                yield
            d = lax.dot_general(v, jnp.concatenate(ps, axis=0), (((1,), (0,)), ((), ())), preferred_element_type=jnp.float32)
            acc = d if acc is None else acc + d
        l = jnp.sum(l8, axis=0, keepdims=True)
        obuf[i, h] = (acc * (1.0 / l)).astype(jnp.bfloat16)
        lbuf[i, h:h + 1, :] = m + jnp.log2(l)
        yield

    def run(*gens):
        live = list(gens)
        while live:
            for g in list(live):
                try:
                    next(g)
                except StopIteration:
                    live.remove(g)

    pair = heads // 2

    def send_far(i, ds):
        return [remote(obuf.at[i, pl.ds(t * pair, pair)], d2o.at[t, ds], a2_send.at[0, t, ds], d2_recv.at[0, t, ds], device(d, 0, core))
                for t, d in ((0, 1), (1, back))] + [
                remote(lbuf.at[i], d2l.at[t, ds], a2_send.at[1, t, ds], d2_recv.at[1, t, ds], device(d, 0, core)) for t, d in ((0, 1), (1, back))]

    def send_near(i, t, ds):
        d = (1, back)[t]
        return [remote(obuf.at[i], aro.at[t, ds], a_send.at[0, t, ds], ar_recv.at[0, t, ds], device(d, 0, core)),
                remote(lbuf.at[i], arl.at[t, ds], a_send.at[1, t, ds], ar_recv.at[1, t, ds], device(d, 0, core))]

    def add_far(i, t, ds):
        for c in send_far(i, ds)[t::2]:
            c.wait_recv()
        for u in range(pair):
            h = t * pair + u
            o, lse = merge([(obuf[i, h], lbuf[i, h:h + 1, :]), (d2o[t, ds, u], d2l[t, ds, h:h + 1, :])])
            obuf[i, h] = o.astype(jnp.bfloat16)
            lbuf[i, h:h + 1, :] = lse

    def send_home(ds, halves):
        return [c for t in halves for c in (
            remote(bo.at[ds, t], fo.at[core, ds], b_send.at[0, t, ds], b_recv.at[0, core, ds], device(0, ds, t)),
            remote(bl.at[ds, t], fl.at[core, ds], b_send.at[1, t, ds], b_recv.at[1, core, ds], device(0, ds, t)))]

    def gather_row(i, ds):
        for t in (0, 1):
            for c in send_near(0, t, ds):
                c.wait_recv()
        for h in range(heads):
            o, lse = merge([(obuf[i, h], lbuf[i, h:h + 1, :])] + [(aro[t, ds, h], arl[t, ds, h:h + 1, :]) for t in (0, 1)])
            o = o.astype(jnp.bfloat16)
            for t in (0, 1):
                bo[ds, t, h] = o[:, t * half_cols:(t + 1) * half_cols]
                bl[ds, t, h:h + 1, :] = lse[:, t * half_cols:(t + 1) * half_cols]

    found = []
    run(scores(0, 0, s0, found))

    def body(i, m):
        for at, (waits, starts) in plan.items():
            @pl.when(i == at)
            def _():
                for w in waits:
                    got(*w)
                for c in starts:
                    c.start()
        nxt = i + 1 - (i + 1) // n_blocks
        for h in range(heads):
            found = []
            last = h + 1 == heads
            run(values(i, h, bufs[h % 2], m), scores(nxt if last else i, 0 if last else h + 1, bufs[(h + 1) % 2], found))
            m = found[0]
        df, ds = place(i)

        @pl.when(df == 2)
        def _():
            for c in send_far(i, ds):
                c.start()

        @pl.when(df == 1)
        def _():
            add_far(i, 0, ds)
            for c in send_near(i, 0, ds):
                c.start()

        @pl.when(df == back)
        def _():
            add_far(i, 1, ds)
            for c in send_near(i, 1, ds):
                c.start()

        @pl.when((i >= n_blocks - side) & (i < n_blocks - 1))
        def _():
            n = i - (n_blocks - side)
            ds = gray(n + 1)
            gather_row(n + (n_blocks - side) * (n // 2), ds)
            for c in send_home(ds, (0, 1)):
                c.start()
        return m

    lax.fori_loop(0, n_blocks, body, found[0])
    gather_row(n_blocks - 1, 0)
    to_sibling = [remote(bo.at[0, other], fo.at[core, 0], b_send.at[0, 0, 0], b_recv.at[0, core, 0], device(0, 0, other)),
                  remote(bl.at[0, other], fl.at[core, 0], b_send.at[1, 0, 0], b_recv.at[1, core, 0], device(0, 0, other))]
    for c in to_sibling:
        c.start()
    fo[core, 0] = bo[0, core]
    fl[core, 0] = bl[0, core]

    for ds in range(1, side):
        for k in (0, 1):
            remote(bo.at[ds, k], fo.at[k, ds], b_send.at[0, 0, 0], b_recv.at[0, k, ds], device(0, 0, core)).wait_recv()
            remote(bl.at[ds, k], fl.at[k, ds], b_send.at[0, 0, 0], b_recv.at[1, k, ds], device(0, 0, core)).wait_recv()
    remote(bo.at[0, 0], fo.at[other, 0], b_send.at[0, 0, 0], b_recv.at[0, other, 0], device(0, 0, core)).wait_recv()
    remote(bl.at[0, 0], fl.at[other, 0], b_send.at[0, 0, 0], b_recv.at[1, other, 0], device(0, 0, core)).wait_recv()
    for k in (0, 1):
        for h in range(heads):
            o, lse = merge([(fo[k, d, h], fl[k, d, h:h + 1, :]) for d in range(side)])
            o = o.T
            for g in range(ratio):
                ostage[pl.ds((k * heads + h) * ratio + g, tok, stride=kv_heads * ratio), :] = o[g * tok:(g + 1) * tok]
            lstage[k * heads + h:k * heads + h + 1, :] = lse * LN2
    out_ref[...] = ostage[...].astype(jnp.bfloat16)
    lse = lstage[:kv_heads, :]
    for g in range(ratio):
        lstage[pl.ds(kv_heads + g, kv_heads, stride=ratio), :] = lse if g == 0 else pltpu.roll(lse, half_cols - g * tok, 1)
    lse_ref[...] = lstage[kv_heads:kv_heads * (ratio + 1), :].T[:tok]

    for c in swaps + sends + to_sibling + [swap_q]:
        c.wait_send()
    for ds in range(side):
        for c in send_far(0, ds) + send_near(0, 0, ds) + send_near(0, 1, ds):
            c.wait_send()
    for ds in range(1, side):
        for c in send_home(ds, (0, 1)):
            c.wait_send()


def solution(mesh):
    groups = mesh.shape['cp']
    side = math.isqrt(groups // 2)
    tok_spec = P(('dp', 'cp'))

    def local_attend(queries, key_new, value_new, key_cache, value_cache, prefix_len):
        tok, heads, dim = queries.shape
        cache_len, kv_heads = key_cache.shape[:2]
        ratio = heads // kv_heads
        half = kv_heads // 2
        rows = tok * ratio
        rows_pad = rows + -rows % 128
        new_pad = -tok % 16
        n_new = tok + new_pad
        keys = 2 * (cache_len + n_new)
        chunk = cache_len // 4
        n_blocks = side * side
        bf, f32 = jnp.bfloat16, jnp.float32
        cols = 2 * rows_pad
        dma = pltpu.SemaphoreType.DMA
        out, lse = pl.pallas_call(
            functools.partial(attend, side, tok, ratio, cache_len),
            in_specs=[pl.BlockSpec(memory_space=pltpu.SMEM)] + [pl.BlockSpec(memory_space=pl.ANY)] * 5,
            out_specs=[pl.BlockSpec(memory_space=pltpu.VMEM)] * 2,
            out_shape=[jax.ShapeDtypeStruct((tok * heads, dim), bf), jax.ShapeDtypeStruct((tok, heads), f32)],
            scratch_shapes=[
                pltpu.VMEM((tok * heads, dim), bf), pltpu.VMEM((tok * kv_heads, dim), bf), pltpu.VMEM((tok * kv_heads, dim), bf),
                pltpu.VMEM((cache_len * kv_heads, dim), bf), pltpu.VMEM((cache_len * kv_heads, dim), bf),
                pltpu.VMEM((2, chunk * kv_heads, dim), f32), pltpu.VMEM((2, half, rows_pad, dim), bf),
                pltpu.VMEM((tok * heads, dim), f32), pltpu.VMEM((kv_heads * (ratio + 1), rows_pad), f32),
                pltpu.VMEM((2, cache_len, 128), f32),
                pltpu.VMEM((keys, cols), f32), pltpu.VMEM((keys, cols), f32),
                pltpu.VMEM((n_blocks, 2, half, rows_pad, dim), bf),
                pltpu.VMEM((3, half, cache_len, dim), bf), pltpu.VMEM((3, half, dim, cache_len), bf),
                pltpu.VMEM((3, half, n_new, dim), bf), pltpu.VMEM((3, half, n_new, dim), bf),
                pltpu.VMEM((half, 2 * n_new, dim), bf), pltpu.VMEM((half, dim, 2 * n_new), bf),
                pltpu.VMEM((n_blocks, half, dim, cols), bf), pltpu.VMEM((n_blocks, half, cols), f32),
                pltpu.VMEM((2, side, half // 2, dim, cols), bf), pltpu.VMEM((2, side, half, cols), f32),
                pltpu.VMEM((2, side, half, dim, cols), bf), pltpu.VMEM((2, side, half, cols), f32),
                pltpu.VMEM((side, 2, half, dim, rows_pad), bf), pltpu.VMEM((side, 2, half, rows_pad), f32),
                pltpu.VMEM((2, side, half, dim, rows_pad), bf), pltpu.VMEM((2, side, half, rows_pad), f32),
                dma((5, 4)), dma((n_blocks, 2)), dma((40,)), dma((3,)), dma((2, 5)), dma((2, 5)), dma,
                dma((2, 2, side)), dma((2, 2, side)), dma((2, 2, side)), dma((2, 2, side)), dma((2, 2, side)), dma((2, 2, side)),
            ],
            compiler_params=pltpu.CompilerParams(collective_id=0, has_side_effects=True, vmem_limit_bytes=60 * 1024 * 1024),
            name='attend',
        )(prefix_len, *[a.reshape(-1, dim) for a in (queries, key_new, value_new, key_cache, value_cache)])
        return out.reshape(tok, heads, dim), lse

    return jax.shard_map(local_attend, mesh=mesh, in_specs=(tok_spec, tok_spec, tok_spec, tok_spec, tok_spec, P('dp')), out_specs=(tok_spec, tok_spec), check_vma=False)
```

```python
import functools
import math

import jax
import jax.numpy as jnp
from jax import lax
from jax.experimental import pallas as pl
from jax.experimental.pallas import tpu as pltpu
from jax.sharding import PartitionSpec as P

MASK_FILL = -1e30
LOG2E = math.log2(math.e)
LN2 = math.log(2.0)
QK_CHUNK = 512
PV_CHUNK = 256
ROW_STEP = 16
SLOTS = 1
ORDER = (1, 10, 30, 0, 3, 20, 11, 23, 21, 12, 22, 13, 31, 32, 33, 2)
PLAN = {
    0: (302, 3003, 1003, 3002, 1002, 3000,),
    1: (1012, 3013, 1013, 113, 3012, 1011,),
    3: (2002, 2003,),
    4: (2012, 3302, 2013,),
    5: (1302, 3113, 1113,),
    6: (2302, 10000,),
    7: (2113,),
    8: (10003,),
    9: (10001, 20000, 20010,),
    11: (10002, 20001,),
    12: (20003,),
    13: (20002, 20011,),
    14: (20012,),
    15: (20013,),
    16: (30001, 30002, 30003,),
}


def gray(p):
    return p + p // 2 - 2 * (p // 3)


def merge(parts):
    top = functools.reduce(jnp.maximum, [lse for _, lse in parts])
    weights = [jnp.exp2(lse - top) for _, lse in parts]
    total = functools.reduce(jnp.add, weights)
    inv = 1.0 / total
    out = functools.reduce(jnp.add, [o.astype(jnp.float32) * (w * inv) for (o, _), w in zip(parts, weights)])
    return out, top + jnp.log2(total)


def attend(side, tok, ratio, cache_len, prefix_ref, q_hbm, kn_hbm, vn_hbm, k_hbm, v_hbm, out_ref, lse_ref,
           qraw, knraw, vnraw, kraw, vraw, stage, qst, ostage, lstage, bias_ref, s0, s1, qbuf, kbuf, vbuf, kx, vx, kcat, vcat, obuf, lbuf, d2o, d2l, aro, arl, bo, bl, fo, fl,
           loads, rq, sq, kv_loc, kv_send, kv_recv, q_swap, d2_recv, ar_recv, a_send, a2_send, b_recv, b_send):
    heads, dim = kbuf.shape[1], kbuf.shape[3]
    n_new = kx.shape[2]
    half_cols = qbuf.shape[3]
    cols = 2 * half_cols
    n_blocks = side * side
    scale = LOG2E * dim ** -0.5
    me = lax.axis_index('cp')
    core = me % 2
    other = 1 - core
    chip = me // 2
    y, x = chip // side, chip % side
    f = y * other + x * core
    s = x * other + y * core
    f_unit = side * other + core
    s_unit = side * core + other

    def slot(df, ds):
        return ((f + df) % side) * f_unit + ((s + ds) % side) * s_unit

    def device(df, ds, which):
        return {'cp': slot(df, ds) * 2 + which}

    def remote(src, dst, send, recv, dev):
        return pltpu.make_async_remote_copy(src_ref=src, dst_ref=dst, send_sem=send, recv_sem=recv, device_id=dev, device_id_type=pl.DeviceIdType.MESH)

    peers = [device(0, 0, other), device(1, 0, core), device(side - 1, 0, core)]
    for d in range(1, side):
        peers += [device(0, d, core), device(0, d, other), device(d, 0, other)]
    barrier = pltpu.get_barrier_semaphore()
    for dev in peers:
        pl.semaphore_signal(barrier, inc=1, device_id=dev, device_id_type=pl.DeviceIdType.MESH)

    mine = slot(0, 0)
    kv_heads = 2 * heads
    chunk = stage.shape[1] // kv_heads
    n_chunks = cache_len // chunk
    small = [pltpu.make_async_copy(src, dst, loads.at[n, 0]) for n, (src, dst) in enumerate(((q_hbm, qraw), (kn_hbm, knraw), (vn_hbm, vnraw)))]

    def raw_copy(n, c):
        rows = pl.ds(pl.multiple_of(c * chunk * kv_heads, chunk * kv_heads), chunk * kv_heads)
        src, dst = ((k_hbm, kraw), (v_hbm, vraw))[n]
        return pltpu.make_async_copy(src.at[rows], dst.at[rows], loads.at[3 + n, c])

    for c in small:
        c.start()
    for c in range(n_chunks):
        for n in (0, 1):
            raw_copy(n, c).start()

    for n, holder in enumerate((core, other)):
        pos = lax.broadcasted_iota(jnp.int32, (cache_len, 128), 0) + (2 * chip + holder) * cache_len
        bias_ref[n] = jnp.where(pos < prefix_ref[0], 0.0, MASK_FILL)

    small[0].wait()
    ostage[...] = qraw[...].astype(jnp.float32)
    for h in range(kv_heads):
        rows = [ostage[pl.ds(h * ratio + g, tok, stride=kv_heads * ratio), :] for g in range(ratio)]
        rows.append(jnp.zeros((half_cols - tok * ratio, dim), jnp.float32))
        qst[h // heads, h % heads] = jnp.concatenate(rows, axis=0).astype(jnp.bfloat16)

    small[1].wait()
    small[2].wait()
    stage[0, :tok * kv_heads] = knraw[...].astype(jnp.float32)
    stage[1, :tok * kv_heads] = vnraw[...].astype(jnp.float32)
    blank = jnp.zeros((n_new - tok, dim), jnp.float32)
    for h in range(kv_heads):
        new_k = jnp.concatenate([stage[0, pl.ds(h, tok, stride=kv_heads), :], blank], axis=0)
        new_v = jnp.concatenate([stage[1, pl.ds(h, tok, stride=kv_heads), :], blank], axis=0)
        kx[h // heads, h % heads] = new_k.astype(jnp.bfloat16)
        vx[h // heads, h % heads] = new_v.astype(jnp.bfloat16)

    pl.semaphore_wait(barrier, len(peers))
    local_q = pltpu.make_async_copy(qst.at[core], qbuf.at[mine, core], kv_loc.at[0])
    local_q.start()
    swap_q = remote(qst.at[other], qbuf.at[mine, core], q_swap, rq.at[mine, core], device(0, 0, other))
    swap_q.start()

    swap_new = [remote(b.at[other], b.at[2], kv_send.at[n, n_chunks], kv_recv.at[n, n_chunks], device(0, 0, other)) for n, b in enumerate((kx, vx))]
    for c in swap_new:
        c.start()

    def swap(c):
        at = pl.ds(c * chunk if isinstance(c, int) else pl.multiple_of(c * chunk, chunk), chunk)
        return [remote(kbuf.at[other, :, at, :], kbuf.at[2, :, at, :], kv_send.at[0, c], kv_recv.at[0, c], device(0, 0, other)),
                remote(vbuf.at[other, :, :, at], vbuf.at[2, :, :, at], kv_send.at[1, c], kv_recv.at[1, c], device(0, 0, other))]

    sends = []

    def piece(df, ds, j, to_df, to_ds):
        where = slot(df, ds)
        c = remote(qbuf.at[where, j], qbuf.at[where, j], sq.at[len(sends)], rq.at[where, j], device(to_df, to_ds, core))
        sends.append(len(sends))
        return c

    def got(df, ds, j):
        where = slot(df, ds)
        remote(qbuf.at[where, j], qbuf.at[where, j], sq.at[0], rq.at[where, j], device(0, 0, core)).wait_recv()

    back = side - 1
    local_q.wait()
    around = [(1, 0), (back, 0), (0, 1), (0, back)]
    first = [piece(0, 0, core, a, b) for a, b in around]
    for c in first:
        c.start()
    second = [piece(0, 0, other, a, b) for a, b in around]

    def relayout(c, carry):
        @pl.when(c == 1)
        def _():
            got(0, 0, other)
            for d in second:
                d.start()

        @pl.when(c > 0)
        def _():
            for d in swap(c - 1):
                d.start()

        rows = pl.ds(pl.multiple_of(c * chunk * kv_heads, chunk * kv_heads), chunk * kv_heads)
        at = pl.ds(pl.multiple_of(c * chunk, chunk), chunk)
        raw_copy(0, c).wait()
        raw_copy(1, c).wait()
        stage[0] = kraw[rows, :].astype(jnp.float32)
        stage[1] = vraw[rows, :].astype(jnp.float32)
        for h in range(kv_heads):
            kbuf[h // heads, h % heads, at, :] = stage[0, pl.ds(h, chunk, stride=kv_heads), :].astype(jnp.bfloat16)
            vbuf[h // heads, h % heads, :, at] = stage[1, pl.ds(h, chunk, stride=kv_heads), :].T.astype(jnp.bfloat16)
        return carry

    lax.fori_loop(0, n_chunks, relayout, 0)
    swaps = [d for c in range(n_chunks) for d in swap(c)]
    for d in swaps[-2:]:
        d.start()
    swaps += swap_new

    seen = {(0, 0, 0), (0, 0, 1)}

    def want(df, ds, j):
        if (df, ds, j) not in seen:
            seen.add((df, ds, j))
            got(df, ds, j)

    order = [divmod(a, 10) for a in ORDER]

    def q_piece(code):
        return code // 1000, code // 100 % 10, code // 10 % 10

    def act(code):
        kind, rest = divmod(code, 10000)
        if kind == 0:
            want(*q_piece(code))
            piece(*q_piece(code), *around[code % 10]).start()
        elif kind == 1:
            for d in send_far(order.index((2, rest)), rest):
                d.start()
        elif kind == 2:
            t, ds = divmod(rest, 10)
            i = order.index(((1, back)[t], ds))
            add_far(i, t, ds)
            for d in send_near(i, t, ds):
                d.start()
        else:
            gather_row(order.index((0, rest)), rest)
            for d in send_home(rest, (0, 1)):
                d.start()

    def slot_run(n, fresh):
        for w in fresh:
            got(*w)
        for code in PLAN.get(n, ()):
            act(code)

    pair = heads // 2

    def send_far(i, ds):
        return [remote(obuf.at[i, pl.ds(t * pair, pair)], d2o.at[t, ds], a2_send.at[0, t, ds], d2_recv.at[0, t, ds], device(d, 0, core))
                for t, d in ((0, 1), (1, back))] + [
                remote(lbuf.at[i], d2l.at[t, ds], a2_send.at[1, t, ds], d2_recv.at[1, t, ds], device(d, 0, core)) for t, d in ((0, 1), (1, back))]

    def send_near(i, t, ds):
        d = (1, back)[t]
        return [remote(obuf.at[i], aro.at[t, ds], a_send.at[0, t, ds], ar_recv.at[0, t, ds], device(d, 0, core)),
                remote(lbuf.at[i], arl.at[t, ds], a_send.at[1, t, ds], ar_recv.at[1, t, ds], device(d, 0, core))]

    def add_far(i, t, ds):
        for c in send_far(i, ds)[t::2]:
            c.wait_recv()
        for u in range(pair):
            h = t * pair + u
            o, lse = merge([(obuf[i, h], lbuf[i, h:h + 1, :]), (d2o[t, ds, u], d2l[t, ds, h:h + 1, :])])
            obuf[i, h] = o.astype(jnp.bfloat16)
            lbuf[i, h:h + 1, :] = lse

    def send_home(ds, halves):
        return [c for t in halves for c in (
            remote(bo.at[ds, t], fo.at[core, ds], b_send.at[0, t, ds], b_recv.at[0, core, ds], device(0, ds, t)),
            remote(bl.at[ds, t], fl.at[core, ds], b_send.at[1, t, ds], b_recv.at[1, core, ds], device(0, ds, t)))]

    def gather_row(i, ds):
        for t in (0, 1):
            for c in send_near(0, t, ds):
                c.wait_recv()
        for h in range(heads):
            o, lse = merge([(obuf[i, h], lbuf[i, h:h + 1, :])] + [(aro[t, ds, h], arl[t, ds, h:h + 1, :]) for t in (0, 1)])
            o = o.astype(jnp.bfloat16)
            for t in (0, 1):
                bo[ds, t, h] = o[:, t * half_cols:(t + 1) * half_cols]
                bl[ds, t, h:h + 1, :] = lse[:, t * half_cols:(t + 1) * half_cols]

    slot_run(-1, ())
    for d in swaps:
        d.wait_recv()

    for h in range(heads):
        kcat[h] = jnp.concatenate([kx[core, h], kx[2, h]], axis=0)
        vcat[h] = jnp.concatenate([vx[core, h], vx[2, h]], axis=0).astype(jnp.float32).T.astype(jnp.bfloat16)

    col = lax.broadcasted_iota(jnp.int32, (1, cols), 1)
    row = col - jnp.where(col >= half_cols, half_cols, 0)
    for g in range(ratio):
        row = row - jnp.where(row >= tok, tok, 0)
    q_tok = row + jnp.where(col >= half_cols, tok, 0)

    def digit(axis, i):
        low, high = (sum(order[first + k][axis] * side ** k for k in range(8)) for first in (0, 8))
        k = i % 8
        power = (1 + (side - 1) * (k % 2)) * (1 + (side ** 2 - 1) * ((k // 2) % 2)) * (1 + (side ** 4 - 1) * (k // 4))
        return ((low + (high - low) * (i // 8)) // power) % side

    def place(i):
        return digit(0, i), digit(1, i)

    bufs = (s0, s1)
    tiles = [(n, a) for n in (0, 1) for a in range(0, cache_len, QK_CHUNK)]

    def scores(i, h, s_ref, found):
        df, ds = place(i)
        where = slot(df, ds)
        q = jnp.concatenate([qbuf[where, 0, h], qbuf[where, 1, h]], axis=0)
        m8 = jnp.full((8, cols), MASK_FILL, jnp.float32)
        for n, a in tiles + [(2, 0)]:
            k = kcat[h] if n == 2 else kbuf[(core, 2)[n], h, a:a + QK_CHUNK, :]
            sc = lax.dot_general(k, q, (((1,), (1,)), ((), ())), preferred_element_type=jnp.float32)
            for r in range(0, k.shape[0], ROW_STEP):
                t = sc[r:r + ROW_STEP] * scale
                if n < 2:
                    bias = bias_ref[n, a + r:a + r + ROW_STEP, :]
                    t = t + jnp.concatenate([bias, bias], axis=1)
                else:
                    step = lax.broadcasted_iota(jnp.int32, t.shape, 0) + r % n_new
                    first_key = (2 * chip + (core, other)[r // n_new]) * tok - 2 * where * tok
                    t = jnp.where((first_key + step <= q_tok) & (step < tok), t, MASK_FILL)
                at = n * cache_len + a + r
                s_ref[at:at + ROW_STEP, :] = t
                for u in range(0, ROW_STEP, 8):
                    m8 = jnp.maximum(m8, t[u:u + 8])
                yield
        found.append(jnp.max(m8, axis=0, keepdims=True))

    def values(i, h, s_ref, m):
        l8 = jnp.zeros((8, cols), jnp.float32)
        acc = None
        for n, a in [(n, a) for n in (0, 1) for a in range(0, cache_len, PV_CHUNK)] + [(2, 0)]:
            v = vcat[h] if n == 2 else vbuf[(core, 2)[n], h, :, a:a + PV_CHUNK]
            ps = []
            for r in range(0, v.shape[1], ROW_STEP):
                at = n * cache_len + a + r
                p = jnp.exp2(s_ref[at:at + ROW_STEP, :] - m)
                for u in range(0, ROW_STEP, 8):
                    l8 = l8 + p[u:u + 8]
                ps.append(p.astype(jnp.bfloat16))
                yield
            d = lax.dot_general(v, jnp.concatenate(ps, axis=0), (((1,), (0,)), ((), ())), preferred_element_type=jnp.float32)
            acc = d if acc is None else acc + d
        l = jnp.sum(l8, axis=0, keepdims=True)
        obuf[i, h] = (acc * (1.0 / l)).astype(jnp.bfloat16)
        lbuf[i, h:h + 1, :] = m + jnp.log2(l)
        yield

    def run(*gens):
        live = list(gens)
        while live:
            for g in list(live):
                try:
                    next(g)
                except StopIteration:
                    live.remove(g)

    for j in (0, 1):
        want(*order[0], j)
    found = []
    run(scores(0, 0, s0, found))

    def body(i, m):
        nxt = i + 1 - (i + 1) // n_blocks
        for h in range(heads):
            if h * SLOTS % heads == 0:
                at = h * SLOTS // heads
                for part in range(0, n_blocks, side):
                    def some(part=part):
                        for k in range(part, part + side):
                            if (k, at) in works:
                                pl.when(i == k)(works[k, at])
                    pl.when(i // side == part // side)(some)
            found = []
            last = h + 1 == heads
            run(values(i, h, bufs[h % 2], m), scores(nxt if last else i, 0 if last else h + 1, bufs[(h + 1) % 2], found))
            m = found[0]
        return m

    works = {}
    for n in range(n_blocks * SLOTS):
        fresh = []
        if n % SLOTS == SLOTS - 1 and n // SLOTS + 1 < n_blocks:
            fresh += [(*order[n // SLOTS + 1], j) for j in (0, 1)]
        fresh += [q_piece(code) for code in PLAN.get(n, ()) if code < 10000]
        fresh = [w for w in dict.fromkeys(fresh) if w not in seen]
        seen.update(fresh)
        if fresh or n in PLAN:
            works[divmod(n, SLOTS)] = functools.partial(slot_run, n, fresh)

    lax.fori_loop(0, n_blocks, body, found[0])
    slot_run(n_blocks * SLOTS, ())
    gather_row(order.index((0, 0)), 0)
    to_sibling = [remote(bo.at[0, other], fo.at[core, 0], b_send.at[0, 0, 0], b_recv.at[0, core, 0], device(0, 0, other)),
                  remote(bl.at[0, other], fl.at[core, 0], b_send.at[1, 0, 0], b_recv.at[1, core, 0], device(0, 0, other))]
    for c in to_sibling:
        c.start()
    fo[core, 0] = bo[0, core]
    fl[core, 0] = bl[0, core]

    for ds in range(1, side):
        for k in (0, 1):
            remote(bo.at[ds, k], fo.at[k, ds], b_send.at[0, 0, 0], b_recv.at[0, k, ds], device(0, 0, core)).wait_recv()
            remote(bl.at[ds, k], fl.at[k, ds], b_send.at[0, 0, 0], b_recv.at[1, k, ds], device(0, 0, core)).wait_recv()
    remote(bo.at[0, 0], fo.at[other, 0], b_send.at[0, 0, 0], b_recv.at[0, other, 0], device(0, 0, core)).wait_recv()
    remote(bl.at[0, 0], fl.at[other, 0], b_send.at[0, 0, 0], b_recv.at[1, other, 0], device(0, 0, core)).wait_recv()
    for k in (0, 1):
        for h in range(heads):
            o, lse = merge([(fo[k, d, h], fl[k, d, h:h + 1, :]) for d in range(side)])
            o = o.T
            for g in range(ratio):
                ostage[pl.ds((k * heads + h) * ratio + g, tok, stride=kv_heads * ratio), :] = o[g * tok:(g + 1) * tok]
            lstage[k * heads + h:k * heads + h + 1, :] = lse * LN2
    out_ref[...] = ostage[...].astype(jnp.bfloat16)
    lse = lstage[:kv_heads, :]
    for g in range(ratio):
        lstage[pl.ds(kv_heads + g, kv_heads, stride=ratio), :] = lse if g == 0 else pltpu.roll(lse, half_cols - g * tok, 1)
    lse_ref[...] = lstage[kv_heads:kv_heads * (ratio + 1), :].T[:tok]

    for c in swaps + to_sibling + [swap_q] + [remote(qbuf.at[mine, 0], qbuf.at[mine, 0], sq.at[n], rq.at[mine, 0], device(0, 0, core)) for n in sends]:
        c.wait_send()
    for ds in range(side):
        for c in send_far(0, ds) + send_near(0, 0, ds) + send_near(0, 1, ds):
            c.wait_send()
    for ds in range(1, side):
        for c in send_home(ds, (0, 1)):
            c.wait_send()


def solution(mesh):
    groups = mesh.shape['cp']
    side = math.isqrt(groups // 2)
    tok_spec = P(('dp', 'cp'))

    def local_attend(queries, key_new, value_new, key_cache, value_cache, prefix_len):
        tok, heads, dim = queries.shape
        cache_len, kv_heads = key_cache.shape[:2]
        ratio = heads // kv_heads
        half = kv_heads // 2
        rows = tok * ratio
        rows_pad = rows + -rows % 128
        new_pad = -tok % 16
        n_new = tok + new_pad
        keys = 2 * (cache_len + n_new)
        chunk = cache_len // 4
        n_blocks = side * side
        bf, f32 = jnp.bfloat16, jnp.float32
        cols = 2 * rows_pad
        dma = pltpu.SemaphoreType.DMA
        out, lse = pl.pallas_call(
            functools.partial(attend, side, tok, ratio, cache_len),
            in_specs=[pl.BlockSpec(memory_space=pltpu.SMEM)] + [pl.BlockSpec(memory_space=pl.ANY)] * 5,
            out_specs=[pl.BlockSpec(memory_space=pltpu.VMEM)] * 2,
            out_shape=[jax.ShapeDtypeStruct((tok * heads, dim), bf), jax.ShapeDtypeStruct((tok, heads), f32)],
            scratch_shapes=[
                pltpu.VMEM((tok * heads, dim), bf), pltpu.VMEM((tok * kv_heads, dim), bf), pltpu.VMEM((tok * kv_heads, dim), bf),
                pltpu.VMEM((cache_len * kv_heads, dim), bf), pltpu.VMEM((cache_len * kv_heads, dim), bf),
                pltpu.VMEM((2, chunk * kv_heads, dim), f32), pltpu.VMEM((2, half, rows_pad, dim), bf),
                pltpu.VMEM((tok * heads, dim), f32), pltpu.VMEM((kv_heads * (ratio + 1), rows_pad), f32),
                pltpu.VMEM((2, cache_len, 128), f32),
                pltpu.VMEM((keys, cols), f32), pltpu.VMEM((keys, cols), f32),
                pltpu.VMEM((n_blocks, 2, half, rows_pad, dim), bf),
                pltpu.VMEM((3, half, cache_len, dim), bf), pltpu.VMEM((3, half, dim, cache_len), bf),
                pltpu.VMEM((3, half, n_new, dim), bf), pltpu.VMEM((3, half, n_new, dim), bf),
                pltpu.VMEM((half, 2 * n_new, dim), bf), pltpu.VMEM((half, dim, 2 * n_new), bf),
                pltpu.VMEM((n_blocks, half, dim, cols), bf), pltpu.VMEM((n_blocks, half, cols), f32),
                pltpu.VMEM((2, side, half // 2, dim, cols), bf), pltpu.VMEM((2, side, half, cols), f32),
                pltpu.VMEM((2, side, half, dim, cols), bf), pltpu.VMEM((2, side, half, cols), f32),
                pltpu.VMEM((side, 2, half, dim, rows_pad), bf), pltpu.VMEM((side, 2, half, rows_pad), f32),
                pltpu.VMEM((2, side, half, dim, rows_pad), bf), pltpu.VMEM((2, side, half, rows_pad), f32),
                dma((5, 4)), dma((n_blocks, 2)), dma((40,)), dma((3,)), dma((2, 5)), dma((2, 5)), dma,
                dma((2, 2, side)), dma((2, 2, side)), dma((2, 2, side)), dma((2, 2, side)), dma((2, 2, side)), dma((2, 2, side)),
            ],
            compiler_params=pltpu.CompilerParams(collective_id=0, has_side_effects=True, vmem_limit_bytes=60 * 1024 * 1024),
            name='attend',
        )(prefix_len, *[a.reshape(-1, dim) for a in (queries, key_new, value_new, key_cache, value_cache)])
        return out.reshape(tok, heads, dim), lse

    return jax.shard_map(local_attend, mesh=mesh, in_specs=(tok_spec, tok_spec, tok_spec, tok_spec, tok_spec, P('dp')), out_specs=(tok_spec, tok_spec), check_vma=False)
```

```python
import functools
import math

import jax
import jax.numpy as jnp
from jax import lax
from jax.experimental import pallas as pl
from jax.experimental.pallas import tpu as pltpu
from jax.sharding import PartitionSpec as P

MASK_FILL = -1e30
LOG2E = math.log2(math.e)
LN2 = math.log(2.0)
QK_CHUNK = 512
PV_CHUNK = 256
ROW_STEP = 16
SLOTS = 1
ORDER = (0, 10, 1, 30, 3, 20, 11, 31, 21, 12, 22, 23, 32, 33, 13, 2)
PLAN = {
    0: (1002, 3002, 3000, 1003, 302, 3003,),
    1: (3013, 1013, 1011, 113, 1012, 3012,),
    3: (1302, 2002, 2003,),
    4: (2013, 2012, 3302,),
    5: (1113, 3113,),
    6: (10000,),
    7: (2302, 2113,),
    9: (10001, 20000, 20010,),
    11: (10002, 20001, 20011,),
    12: (10003,),
    13: (20002, 20012,),
    15: (20013, 20003,),
    16: (30002, 30001, 30003,),
}


def gray(p):
    return p + p // 2 - 2 * (p // 3)


def merge(parts):
    top = functools.reduce(jnp.maximum, [lse for _, lse in parts])
    weights = [jnp.exp2(lse - top) for _, lse in parts]
    total = functools.reduce(jnp.add, weights)
    inv = 1.0 / total
    out = functools.reduce(jnp.add, [o.astype(jnp.float32) * (w * inv) for (o, _), w in zip(parts, weights)])
    return out, top + jnp.log2(total)


def attend(side, tok, ratio, cache_len, prefix_ref, q_hbm, kn_hbm, vn_hbm, k_hbm, v_hbm, out_ref, lse_ref,
           qraw, knraw, vnraw, kraw, vraw, stage, qst, ostage, lstage, bias_ref, s0, s1, qbuf, kbuf, vbuf, kx, vx, kcat, vcat, obuf, lbuf, d2o, d2l, aro, arl, bo, bl, fo, fl,
           loads, rq, sq, kv_loc, kv_send, kv_recv, q_swap, d2_recv, ar_recv, a_send, a2_send, b_recv, b_send, bf_recv, bfo, bfl):
    heads, dim = kbuf.shape[1], kbuf.shape[3]
    n_new = kx.shape[2]
    half_cols = qbuf.shape[3]
    cols = 2 * half_cols
    n_blocks = side * side
    scale = LOG2E * dim ** -0.5
    me = lax.axis_index('cp')
    core = me % 2
    other = 1 - core
    chip = me // 2
    y, x = chip // side, chip % side
    f = y * other + x * core
    s = x * other + y * core
    f_unit = side * other + core
    s_unit = side * core + other

    def slot(df, ds):
        return ((f + df) % side) * f_unit + ((s + ds) % side) * s_unit

    def device(df, ds, which):
        return {'cp': slot(df, ds) * 2 + which}

    def remote(src, dst, send, recv, dev):
        return pltpu.make_async_remote_copy(src_ref=src, dst_ref=dst, send_sem=send, recv_sem=recv, device_id=dev, device_id_type=pl.DeviceIdType.MESH)

    peers = [device(0, 0, other), device(1, 0, core), device(side - 1, 0, core)]
    for d in range(1, side):
        peers += [device(0, d, core), device(0, d, other), device(d, 0, other)]
    barrier = pltpu.get_barrier_semaphore()
    for dev in peers:
        pl.semaphore_signal(barrier, inc=1, device_id=dev, device_id_type=pl.DeviceIdType.MESH)

    mine = slot(0, 0)
    kv_heads = 2 * heads
    chunk = stage.shape[1] // kv_heads
    n_chunks = cache_len // chunk
    small = [pltpu.make_async_copy(src, dst, loads.at[n, 0]) for n, (src, dst) in enumerate(((q_hbm, qraw), (kn_hbm, knraw), (vn_hbm, vnraw)))]

    def raw_copy(n, c):
        rows = pl.ds(pl.multiple_of(c * chunk * kv_heads, chunk * kv_heads), chunk * kv_heads)
        src, dst = ((k_hbm, kraw), (v_hbm, vraw))[n]
        return pltpu.make_async_copy(src.at[rows], dst.at[rows], loads.at[3 + n, c])

    for c in small:
        c.start()
    for c in range(n_chunks):
        for n in (0, 1):
            raw_copy(n, c).start()

    small[0].wait()
    ostage[...] = qraw[...].astype(jnp.float32)
    for h in range(kv_heads):
        rows = [ostage[pl.ds(h * ratio + g, tok, stride=kv_heads * ratio), :] for g in range(ratio)]
        rows.append(jnp.zeros((half_cols - tok * ratio, dim), jnp.float32))
        qst[h // heads, h % heads] = jnp.concatenate(rows, axis=0).astype(jnp.bfloat16)

    pl.semaphore_wait(barrier, len(peers))
    local_q = pltpu.make_async_copy(qst.at[core], qbuf.at[mine, core], kv_loc.at[0])
    local_q.start()
    swap_q = remote(qst.at[other], qbuf.at[mine, core], q_swap, rq.at[mine, core], device(0, 0, other))
    swap_q.start()

    def swap(c):
        at = pl.ds(c * chunk if isinstance(c, int) else pl.multiple_of(c * chunk, chunk), chunk)
        return [remote(kbuf.at[other, :, at, :], kbuf.at[2, :, at, :], kv_send.at[0, c], kv_recv.at[0, c], device(0, 0, other)),
                remote(vbuf.at[other, :, :, at], vbuf.at[2, :, :, at], kv_send.at[1, c], kv_recv.at[1, c], device(0, 0, other))]

    sends = []

    def piece(df, ds, j, to_df, to_ds, held=None):
        where = slot(df, ds)
        c = remote(qbuf.at[where, j] if held is None else held, qbuf.at[where, j], sq.at[len(sends)], rq.at[where, j], device(to_df, to_ds, core))
        sends.append(len(sends))
        return c

    def got(df, ds, j):
        where = slot(df, ds)
        remote(qbuf.at[where, j], qbuf.at[where, j], sq.at[0], rq.at[where, j], device(0, 0, core)).wait_recv()

    back = side - 1
    around = [(1, 0), (back, 0), (0, 1), (0, back)]
    for a, b in around:
        piece(0, 0, core, a, b, qst.at[core]).start()
    for n, holder in enumerate((core, other)):
        pos = lax.broadcasted_iota(jnp.int32, (cache_len, 128), 0) + (2 * chip + holder) * cache_len
        bias_ref[n] = jnp.where(pos < prefix_ref[0], 0.0, MASK_FILL)

    small[1].wait()
    small[2].wait()
    stage[0, :tok * kv_heads] = knraw[...].astype(jnp.float32)
    stage[1, :tok * kv_heads] = vnraw[...].astype(jnp.float32)
    blank = jnp.zeros((n_new - tok, dim), jnp.float32)
    for h in range(kv_heads):
        new_k = jnp.concatenate([stage[0, pl.ds(h, tok, stride=kv_heads), :], blank], axis=0)
        new_v = jnp.concatenate([stage[1, pl.ds(h, tok, stride=kv_heads), :], blank], axis=0)
        kx[h // heads, h % heads] = new_k.astype(jnp.bfloat16)
        vx[h // heads, h % heads] = new_v.astype(jnp.bfloat16)

    swap_new = [remote(b.at[other], b.at[2], kv_send.at[n, n_chunks], kv_recv.at[n, n_chunks], device(0, 0, other)) for n, b in enumerate((kx, vx))]
    for c in swap_new:
        c.start()

    second = [piece(0, 0, other, a, b) for a, b in around]

    def relayout(c, carry):
        @pl.when(c == 1)
        def _():
            got(0, 0, other)
            for d in second:
                d.start()

        @pl.when(c > 0)
        def _():
            for d in swap(c - 1):
                d.start()

        rows = pl.ds(pl.multiple_of(c * chunk * kv_heads, chunk * kv_heads), chunk * kv_heads)
        at = pl.ds(pl.multiple_of(c * chunk, chunk), chunk)
        raw_copy(0, c).wait()
        raw_copy(1, c).wait()
        stage[0] = kraw[rows, :].astype(jnp.float32)
        stage[1] = vraw[rows, :].astype(jnp.float32)
        for h in range(kv_heads):
            kbuf[h // heads, h % heads, at, :] = stage[0, pl.ds(h, chunk, stride=kv_heads), :].astype(jnp.bfloat16)
            vbuf[h // heads, h % heads, :, at] = stage[1, pl.ds(h, chunk, stride=kv_heads), :].T.astype(jnp.bfloat16)
        return carry

    lax.fori_loop(0, n_chunks, relayout, 0)
    swaps = [d for c in range(n_chunks) for d in swap(c)]
    for d in swaps[-2:]:
        d.start()
    swaps += swap_new

    seen = {(0, 0, 0), (0, 0, 1)}

    def want(df, ds, j):
        if (df, ds, j) not in seen:
            seen.add((df, ds, j))
            got(df, ds, j)

    order = [divmod(a, 10) for a in ORDER]

    def q_piece(code):
        return code // 1000, code // 100 % 10, code // 10 % 10

    def act(code):
        kind, rest = divmod(code, 10000)
        if kind == 0:
            want(*q_piece(code))
            piece(*q_piece(code), *around[code % 10]).start()
        elif kind == 1:
            for d in send_far(order.index((2, rest)), rest):
                d.start()
        elif kind == 2:
            t, ds = divmod(rest, 10)
            i = order.index(((1, back)[t], ds))
            add_far(i, t, ds)
            for d in send_near(i, t, ds):
                d.start()
        else:
            gather_row(order.index((0, rest)), rest)
            for d in send_home(rest):
                d.start()

    def slot_run(n, fresh):
        for w in fresh:
            got(*w)
        for code in PLAN.get(n, ()):
            act(code)

    pair = heads // 2

    def send_far(i, ds):
        return [remote(obuf.at[i, pl.ds(t * pair, pair)], d2o.at[t, ds], a2_send.at[0, t, ds], d2_recv.at[0, t, ds], device(d, 0, core))
                for t, d in ((0, 1), (1, back))] + [
                remote(lbuf.at[i], d2l.at[t, ds], a2_send.at[1, t, ds], d2_recv.at[1, t, ds], device(d, 0, core)) for t, d in ((0, 1), (1, back))]

    def send_near(i, t, ds):
        d = (1, back)[t]
        return [remote(obuf.at[i], aro.at[t, ds], a_send.at[0, t, ds], ar_recv.at[0, t, ds], device(d, 0, core)),
                remote(lbuf.at[i], arl.at[t, ds], a_send.at[1, t, ds], ar_recv.at[1, t, ds], device(d, 0, core))]

    def add_far(i, t, ds):
        for c in send_far(i, ds)[t::2]:
            c.wait_recv()
        for u in range(pair):
            h = t * pair + u
            o, lse = merge([(obuf[i, h], lbuf[i, h:h + 1, :]), (d2o[t, ds, u], d2l[t, ds, h:h + 1, :])])
            obuf[i, h] = o.astype(jnp.bfloat16)
            lbuf[i, h:h + 1, :] = lse

    def send_home(ds):
        if ds == 2:
            return [c for t, d in ((0, 1), (1, back)) for c in (
                remote(bo.at[ds, t], bfo.at[t], b_send.at[0, t, ds], bf_recv.at[0, t], device(0, d, core)),
                remote(bl.at[ds, t], bfl.at[t], b_send.at[1, t, ds], bf_recv.at[1, t], device(0, d, core)))]
        return [c for t in (0, 1) for c in (
            remote(bo.at[ds, t], fo.at[core, ds], b_send.at[0, t, ds], b_recv.at[0, core, ds], device(0, ds, t)),
            remote(bl.at[ds, t], fl.at[core, ds], b_send.at[1, t, ds], b_recv.at[1, core, ds], device(0, ds, t)))]

    def gather_row(i, ds):
        for t in (0, 1):
            for c in send_near(i, t, ds):
                c.wait_recv()
        far = {1: 0, back: 1}.get(ds)
        if far is not None:
            for c in send_home(2)[2 * far:2 * far + 2]:
                c.wait_recv()
        for h in range(heads):
            for t in (0, 1):
                at = slice(t * half_cols, (t + 1) * half_cols)
                parts = [(obuf[i, h, :, at], lbuf[i, h:h + 1, at])] + [(aro[d, ds, h, :, at], arl[d, ds, h:h + 1, at]) for d in (0, 1)]
                if t == far:
                    parts.append((bfo[t, h], bfl[t, h:h + 1, :]))
                o, lse = merge(parts)
                bo[ds, t, h] = o.astype(jnp.bfloat16)
                bl[ds, t, h:h + 1, :] = lse

    slot_run(-1, ())
    local_q.wait()
    for d in swaps:
        d.wait_recv()

    for h in range(heads):
        kcat[h] = jnp.concatenate([kx[core, h], kx[2, h]], axis=0)
        vcat[h] = jnp.concatenate([vx[core, h], vx[2, h]], axis=0).astype(jnp.float32).T.astype(jnp.bfloat16)

    col = lax.broadcasted_iota(jnp.int32, (1, cols), 1)
    row = col - jnp.where(col >= half_cols, half_cols, 0)
    for g in range(ratio):
        row = row - jnp.where(row >= tok, tok, 0)
    q_tok = row + jnp.where(col >= half_cols, tok, 0)

    def digit(axis, i):
        low, high = (sum(order[first + k][axis] * side ** k for k in range(8)) for first in (0, 8))
        k = i % 8
        power = (1 + (side - 1) * (k % 2)) * (1 + (side ** 2 - 1) * ((k // 2) % 2)) * (1 + (side ** 4 - 1) * (k // 4))
        return ((low + (high - low) * (i // 8)) // power) % side

    def place(i):
        return digit(0, i), digit(1, i)

    bufs = (s0, s1)
    tiles = [(n, a) for n in (0, 1) for a in range(0, cache_len, QK_CHUNK)]

    def scores(i, h, s_ref, found):
        df, ds = place(i)
        where = slot(df, ds)
        q = jnp.concatenate([qbuf[where, 0, h], qbuf[where, 1, h]], axis=0)
        m8 = jnp.full((8, cols), MASK_FILL, jnp.float32)
        for n, a in tiles + [(2, 0)]:
            k = kcat[h] if n == 2 else kbuf[(core, 2)[n], h, a:a + QK_CHUNK, :]
            sc = lax.dot_general(k, q, (((1,), (1,)), ((), ())), preferred_element_type=jnp.float32)
            for r in range(0, k.shape[0], ROW_STEP):
                t = sc[r:r + ROW_STEP] * scale
                if n < 2:
                    bias = bias_ref[n, a + r:a + r + ROW_STEP, :]
                    t = t + jnp.concatenate([bias, bias], axis=1)
                else:
                    step = lax.broadcasted_iota(jnp.int32, t.shape, 0) + r % n_new
                    first_key = (2 * chip + (core, other)[r // n_new]) * tok - 2 * where * tok
                    t = jnp.where((first_key + step <= q_tok) & (step < tok), t, MASK_FILL)
                at = n * cache_len + a + r
                s_ref[at:at + ROW_STEP, :] = t
                for u in range(0, ROW_STEP, 8):
                    m8 = jnp.maximum(m8, t[u:u + 8])
                yield
        found.append(jnp.max(m8, axis=0, keepdims=True))

    def values(i, h, s_ref, m):
        l8 = jnp.zeros((8, cols), jnp.float32)
        acc = None
        for n, a in [(n, a) for n in (0, 1) for a in range(0, cache_len, PV_CHUNK)] + [(2, 0)]:
            v = vcat[h] if n == 2 else vbuf[(core, 2)[n], h, :, a:a + PV_CHUNK]
            ps = []
            for r in range(0, v.shape[1], ROW_STEP):
                at = n * cache_len + a + r
                p = jnp.exp2(s_ref[at:at + ROW_STEP, :] - m)
                for u in range(0, ROW_STEP, 8):
                    l8 = l8 + p[u:u + 8]
                ps.append(p.astype(jnp.bfloat16))
                yield
            d = lax.dot_general(v, jnp.concatenate(ps, axis=0), (((1,), (0,)), ((), ())), preferred_element_type=jnp.float32)
            acc = d if acc is None else acc + d
        l = jnp.sum(l8, axis=0, keepdims=True)
        obuf[i, h] = (acc * (1.0 / l)).astype(jnp.bfloat16)
        lbuf[i, h:h + 1, :] = m + jnp.log2(l)
        yield

    def run(*gens):
        live = list(gens)
        while live:
            for g in list(live):
                try:
                    next(g)
                except StopIteration:
                    live.remove(g)

    for j in (0, 1):
        want(*order[0], j)
    found = []
    run(scores(0, 0, s0, found))

    def body(i, m):
        nxt = i + 1 - (i + 1) // n_blocks
        for h in range(heads):
            if h * SLOTS % heads == 0:
                at = h * SLOTS // heads
                for part in range(0, n_blocks, side):
                    def some(part=part):
                        for k in range(part, part + side):
                            if (k, at) in works:
                                pl.when(i == k)(works[k, at])
                    pl.when(i // side == part // side)(some)
            found = []
            last = h + 1 == heads
            run(values(i, h, bufs[h % 2], m), scores(nxt if last else i, 0 if last else h + 1, bufs[(h + 1) % 2], found))
            m = found[0]
        return m

    works = {}
    for n in range(n_blocks * SLOTS):
        fresh = []
        if n % SLOTS == SLOTS - 1 and n // SLOTS + 1 < n_blocks:
            fresh += [(*order[n // SLOTS + 1], j) for j in (0, 1)]
        fresh += [q_piece(code) for code in PLAN.get(n, ()) if code < 10000]
        fresh = [w for w in dict.fromkeys(fresh) if w not in seen]
        seen.update(fresh)
        if fresh or n in PLAN:
            works[divmod(n, SLOTS)] = functools.partial(slot_run, n, fresh)

    lax.fori_loop(0, n_blocks, body, found[0])
    slot_run(n_blocks * SLOTS, ())
    gather_row(order.index((0, 0)), 0)
    to_sibling = [remote(bo.at[0, other], fo.at[core, 0], b_send.at[0, 0, 0], b_recv.at[0, core, 0], device(0, 0, other)),
                  remote(bl.at[0, other], fl.at[core, 0], b_send.at[1, 0, 0], b_recv.at[1, core, 0], device(0, 0, other))]
    for c in to_sibling:
        c.start()
    fo[core, 0] = bo[0, core]
    fl[core, 0] = bl[0, core]

    near = (0, 1, back)
    for ds in near[1:]:
        for k in (0, 1):
            remote(bo.at[ds, k], fo.at[k, ds], b_send.at[0, 0, 0], b_recv.at[0, k, ds], device(0, 0, core)).wait_recv()
            remote(bl.at[ds, k], fl.at[k, ds], b_send.at[0, 0, 0], b_recv.at[1, k, ds], device(0, 0, core)).wait_recv()
    remote(bo.at[0, 0], fo.at[other, 0], b_send.at[0, 0, 0], b_recv.at[0, other, 0], device(0, 0, core)).wait_recv()
    remote(bl.at[0, 0], fl.at[other, 0], b_send.at[0, 0, 0], b_recv.at[1, other, 0], device(0, 0, core)).wait_recv()
    for k in (0, 1):
        for h in range(heads):
            o, lse = merge([(fo[k, d, h], fl[k, d, h:h + 1, :]) for d in near])
            o = o.T
            for g in range(ratio):
                ostage[pl.ds((k * heads + h) * ratio + g, tok, stride=kv_heads * ratio), :] = o[g * tok:(g + 1) * tok]
            lstage[k * heads + h:k * heads + h + 1, :] = lse * LN2
    out_ref[...] = ostage[...].astype(jnp.bfloat16)
    lse = lstage[:kv_heads, :]
    for g in range(ratio):
        lstage[pl.ds(kv_heads + g, kv_heads, stride=ratio), :] = lse if g == 0 else pltpu.roll(lse, half_cols - g * tok, 1)
    lse_ref[...] = lstage[kv_heads:kv_heads * (ratio + 1), :].T[:tok]

    for c in swaps + to_sibling + [swap_q] + [remote(qbuf.at[mine, 0], qbuf.at[mine, 0], sq.at[n], rq.at[mine, 0], device(0, 0, core)) for n in sends]:
        c.wait_send()
    for ds in range(side):
        for c in send_far(0, ds) + send_near(0, 0, ds) + send_near(0, 1, ds):
            c.wait_send()
    for ds in range(1, side):
        for c in send_home(ds):
            c.wait_send()


def solution(mesh):
    groups = mesh.shape['cp']
    side = math.isqrt(groups // 2)
    tok_spec = P(('dp', 'cp'))

    def local_attend(queries, key_new, value_new, key_cache, value_cache, prefix_len):
        tok, heads, dim = queries.shape
        cache_len, kv_heads = key_cache.shape[:2]
        ratio = heads // kv_heads
        half = kv_heads // 2
        rows = tok * ratio
        rows_pad = rows + -rows % 128
        new_pad = -tok % 16
        n_new = tok + new_pad
        keys = 2 * (cache_len + n_new)
        chunk = cache_len // 4
        n_blocks = side * side
        bf, f32 = jnp.bfloat16, jnp.float32
        cols = 2 * rows_pad
        dma = pltpu.SemaphoreType.DMA
        out, lse = pl.pallas_call(
            functools.partial(attend, side, tok, ratio, cache_len),
            in_specs=[pl.BlockSpec(memory_space=pltpu.SMEM)] + [pl.BlockSpec(memory_space=pl.ANY)] * 5,
            out_specs=[pl.BlockSpec(memory_space=pltpu.VMEM)] * 2,
            out_shape=[jax.ShapeDtypeStruct((tok * heads, dim), bf), jax.ShapeDtypeStruct((tok, heads), f32)],
            scratch_shapes=[
                pltpu.VMEM((tok * heads, dim), bf), pltpu.VMEM((tok * kv_heads, dim), bf), pltpu.VMEM((tok * kv_heads, dim), bf),
                pltpu.VMEM((cache_len * kv_heads, dim), bf), pltpu.VMEM((cache_len * kv_heads, dim), bf),
                pltpu.VMEM((2, chunk * kv_heads, dim), f32), pltpu.VMEM((2, half, rows_pad, dim), bf),
                pltpu.VMEM((tok * heads, dim), f32), pltpu.VMEM((kv_heads * (ratio + 1), rows_pad), f32),
                pltpu.VMEM((2, cache_len, 128), f32),
                pltpu.VMEM((keys, cols), f32), pltpu.VMEM((keys, cols), f32),
                pltpu.VMEM((n_blocks, 2, half, rows_pad, dim), bf),
                pltpu.VMEM((3, half, cache_len, dim), bf), pltpu.VMEM((3, half, dim, cache_len), bf),
                pltpu.VMEM((3, half, n_new, dim), bf), pltpu.VMEM((3, half, n_new, dim), bf),
                pltpu.VMEM((half, 2 * n_new, dim), bf), pltpu.VMEM((half, dim, 2 * n_new), bf),
                pltpu.VMEM((n_blocks, half, dim, cols), bf), pltpu.VMEM((n_blocks, half, cols), f32),
                pltpu.VMEM((2, side, half // 2, dim, cols), bf), pltpu.VMEM((2, side, half, cols), f32),
                pltpu.VMEM((2, side, half, dim, cols), bf), pltpu.VMEM((2, side, half, cols), f32),
                pltpu.VMEM((side, 2, half, dim, rows_pad), bf), pltpu.VMEM((side, 2, half, rows_pad), f32),
                pltpu.VMEM((2, side, half, dim, rows_pad), bf), pltpu.VMEM((2, side, half, rows_pad), f32),
                dma((5, 4)), dma((n_blocks, 2)), dma((40,)), dma((3,)), dma((2, 5)), dma((2, 5)), dma,
                dma((2, 2, side)), dma((2, 2, side)), dma((2, 2, side)), dma((2, 2, side)), dma((2, 2, side)), dma((2, 2, side)), dma((2, 2)),
                pltpu.VMEM((2, half, dim, rows_pad), bf), pltpu.VMEM((2, half, rows_pad), f32),
            ],
            compiler_params=pltpu.CompilerParams(collective_id=0, has_side_effects=True, vmem_limit_bytes=60 * 1024 * 1024),
            name='attend',
        )(prefix_len, *[a.reshape(-1, dim) for a in (queries, key_new, value_new, key_cache, value_cache)])
        return out.reshape(tok, heads, dim), lse

    return jax.shard_map(local_attend, mesh=mesh, in_specs=(tok_spec, tok_spec, tok_spec, tok_spec, tok_spec, P('dp')), out_specs=(tok_spec, tok_spec), check_vma=False)
```

```python
import functools
import math

import jax
import jax.numpy as jnp
from jax import lax
from jax.experimental import pallas as pl
from jax.experimental.pallas import tpu as pltpu
from jax.sharding import PartitionSpec as P

MASK_FILL = -1e30
LOG2E = math.log2(math.e)
LN2 = math.log(2.0)
QK_CHUNK = 512
PV_CHUNK = 256
ROW_STEP = 16
SLOTS = 1
ORDER = (0, 10, 1, 30, 3, 20, 11, 31, 21, 12, 22, 23, 32, 33, 13, 2)
PLAN = {
    0: (1002, 3002, 3000, 1003, 302, 3003,),
    1: (3013, 1013, 1011, 113, 1012, 3012,),
    3: (1302, 2002, 2003,),
    4: (2013, 2012, 3302,),
    5: (1113, 3113,),
    6: (10000,),
    7: (2302, 2113,),
    9: (10001, 20000, 20010,),
    11: (10002, 20001, 20011,),
    12: (10003,),
    13: (20002, 20012,),
    15: (20013, 20003,),
    16: (30002, 30001, 30003,),
}


def gray(p):
    return p + p // 2 - 2 * (p // 3)


def merge(parts):
    top = functools.reduce(jnp.maximum, [lse for _, lse in parts])
    weights = [jnp.exp2(lse - top) for _, lse in parts]
    total = functools.reduce(jnp.add, weights)
    inv = 1.0 / total
    out = functools.reduce(jnp.add, [o.astype(jnp.float32) * (w * inv) for (o, _), w in zip(parts, weights)])
    return out, top + jnp.log2(total)


def attend(side, tok, ratio, cache_len, prefix_ref, q_hbm, kn_hbm, vn_hbm, k_hbm, v_hbm, out_ref, lse_ref,
           qraw, knraw, vnraw, kraw, vraw, stage, qst, ostage, lstage, bias_ref, s0, s1, qbuf, kbuf, vbuf, kx, vx, kcat, vcat, obuf, lbuf, d2o, d2l, aro, arl, bo, bl, fo, fl,
           loads, rq, sq, kv_loc, kv_send, kv_recv, q_swap, d2_recv, ar_recv, a_send, a2_send, b_recv, b_send, bf_recv, bfo, bfl):
    heads, dim = kbuf.shape[1], kbuf.shape[3]
    n_new = kx.shape[2]
    half_cols = lbuf.shape[2] // 2
    n_rows = tok * ratio
    lead = [h * n_rows % 16 for h in range(heads)]
    cols = 2 * half_cols
    n_blocks = side * side
    scale = LOG2E * dim ** -0.5
    me = lax.axis_index('cp')
    core = me % 2
    other = 1 - core
    chip = me // 2
    y, x = chip // side, chip % side
    f = y * other + x * core
    s = x * other + y * core
    f_unit = side * other + core
    s_unit = side * core + other

    def slot(df, ds):
        return ((f + df) % side) * f_unit + ((s + ds) % side) * s_unit

    def device(df, ds, which):
        return {'cp': slot(df, ds) * 2 + which}

    def remote(src, dst, send, recv, dev):
        return pltpu.make_async_remote_copy(src_ref=src, dst_ref=dst, send_sem=send, recv_sem=recv, device_id=dev, device_id_type=pl.DeviceIdType.MESH)

    peers = [device(0, 0, other), device(1, 0, core), device(side - 1, 0, core)]
    for d in range(1, side):
        peers += [device(0, d, core), device(0, d, other), device(d, 0, other)]
    barrier = pltpu.get_barrier_semaphore()
    for dev in peers:
        pl.semaphore_signal(barrier, inc=1, device_id=dev, device_id_type=pl.DeviceIdType.MESH)

    mine = slot(0, 0)
    kv_heads = 2 * heads
    chunk = stage.shape[1] // kv_heads
    n_chunks = cache_len // chunk
    small = [pltpu.make_async_copy(src, dst, loads.at[n, 0]) for n, (src, dst) in enumerate(((q_hbm, qraw), (kn_hbm, knraw), (vn_hbm, vnraw)))]

    def raw_copy(n, c):
        rows = pl.ds(pl.multiple_of(c * chunk * kv_heads, chunk * kv_heads), chunk * kv_heads)
        src, dst = ((k_hbm, kraw), (v_hbm, vraw))[n]
        return pltpu.make_async_copy(src.at[rows], dst.at[rows], loads.at[3 + n, c])

    for c in small:
        c.start()
    for c in range(n_chunks):
        for n in (0, 1):
            raw_copy(n, c).start()

    small[0].wait()
    ostage[...] = qraw[...].astype(jnp.float32)
    for n in (0, 1):
        rows = [ostage[pl.ds(h * ratio + g, tok, stride=kv_heads * ratio), :] for h in range(n * heads, (n + 1) * heads) for g in range(ratio)]
        qst[n] = jnp.concatenate(rows, axis=0).astype(jnp.bfloat16)

    pl.semaphore_wait(barrier, len(peers))
    local_q = pltpu.make_async_copy(qst.at[core], qbuf.at[mine, core], kv_loc.at[0])
    local_q.start()
    swap_q = remote(qst.at[other], qbuf.at[mine, core], q_swap, rq.at[mine, core], device(0, 0, other))
    swap_q.start()

    def swap(c):
        at = pl.ds(c * chunk if isinstance(c, int) else pl.multiple_of(c * chunk, chunk), chunk)
        return [remote(kbuf.at[other, :, at, :], kbuf.at[2, :, at, :], kv_send.at[0, c], kv_recv.at[0, c], device(0, 0, other)),
                remote(vbuf.at[other, :, :, at], vbuf.at[2, :, :, at], kv_send.at[1, c], kv_recv.at[1, c], device(0, 0, other))]

    sends = []

    def piece(df, ds, j, to_df, to_ds, held=None):
        where = slot(df, ds)
        c = remote(qbuf.at[where, j] if held is None else held, qbuf.at[where, j], sq.at[len(sends)], rq.at[where, j], device(to_df, to_ds, core))
        sends.append(len(sends))
        return c

    def got(df, ds, j):
        where = slot(df, ds)
        remote(qbuf.at[where, j], qbuf.at[where, j], sq.at[0], rq.at[where, j], device(0, 0, core)).wait_recv()

    back = side - 1
    around = [(1, 0), (back, 0), (0, 1), (0, back)]
    for a, b in around:
        piece(0, 0, core, a, b, qst.at[core]).start()
    for n, holder in enumerate((core, other)):
        pos = lax.broadcasted_iota(jnp.int32, (cache_len, 128), 0) + (2 * chip + holder) * cache_len
        bias_ref[n] = jnp.where(pos < prefix_ref[0], 0.0, MASK_FILL)

    small[1].wait()
    small[2].wait()
    stage[0, :tok * kv_heads] = knraw[...].astype(jnp.float32)
    stage[1, :tok * kv_heads] = vnraw[...].astype(jnp.float32)
    blank = jnp.zeros((n_new - tok, dim), jnp.float32)
    for h in range(kv_heads):
        new_k = jnp.concatenate([stage[0, pl.ds(h, tok, stride=kv_heads), :], blank], axis=0)
        new_v = jnp.concatenate([stage[1, pl.ds(h, tok, stride=kv_heads), :], blank], axis=0)
        kx[h // heads, h % heads] = new_k.astype(jnp.bfloat16)
        vx[h // heads, h % heads] = new_v.astype(jnp.bfloat16)

    swap_new = [remote(b.at[other], b.at[2], kv_send.at[n, n_chunks], kv_recv.at[n, n_chunks], device(0, 0, other)) for n, b in enumerate((kx, vx))]
    for c in swap_new:
        c.start()

    second = [piece(0, 0, other, a, b) for a, b in around]

    def relayout(c, carry):
        @pl.when(c == 1)
        def _():
            got(0, 0, other)
            for d in second:
                d.start()

        @pl.when(c > 0)
        def _():
            for d in swap(c - 1):
                d.start()

        rows = pl.ds(pl.multiple_of(c * chunk * kv_heads, chunk * kv_heads), chunk * kv_heads)
        at = pl.ds(pl.multiple_of(c * chunk, chunk), chunk)
        raw_copy(0, c).wait()
        raw_copy(1, c).wait()
        stage[0] = kraw[rows, :].astype(jnp.float32)
        stage[1] = vraw[rows, :].astype(jnp.float32)
        for h in range(kv_heads):
            kbuf[h // heads, h % heads, at, :] = stage[0, pl.ds(h, chunk, stride=kv_heads), :].astype(jnp.bfloat16)
            vbuf[h // heads, h % heads, :, at] = stage[1, pl.ds(h, chunk, stride=kv_heads), :].T.astype(jnp.bfloat16)
        return carry

    lax.fori_loop(0, n_chunks, relayout, 0)
    swaps = [d for c in range(n_chunks) for d in swap(c)]
    for d in swaps[-2:]:
        d.start()
    swaps += swap_new

    seen = {(0, 0, 0), (0, 0, 1)}

    def want(df, ds, j):
        if (df, ds, j) not in seen:
            seen.add((df, ds, j))
            got(df, ds, j)

    order = [divmod(a, 10) for a in ORDER]

    def q_piece(code):
        return code // 1000, code // 100 % 10, code // 10 % 10

    def act(code):
        kind, rest = divmod(code, 10000)
        if kind == 0:
            want(*q_piece(code))
            piece(*q_piece(code), *around[code % 10]).start()
        elif kind == 1:
            for d in send_far(order.index((2, rest)), rest):
                d.start()
        elif kind == 2:
            t, ds = divmod(rest, 10)
            i = order.index(((1, back)[t], ds))
            add_far(i, t, ds)
            for d in send_near(i, t, ds):
                d.start()
        else:
            gather_row(order.index((0, rest)), rest)
            for d in send_home(rest):
                d.start()

    def slot_run(n, fresh):
        for w in fresh:
            got(*w)
        for code in PLAN.get(n, ()):
            act(code)

    pair = heads // 2

    def send_far(i, ds):
        return [remote(obuf.at[i, pl.ds(t * pair, pair)], d2o.at[t, ds], a2_send.at[0, t, ds], d2_recv.at[0, t, ds], device(d, 0, core))
                for t, d in ((0, 1), (1, back))] + [
                remote(lbuf.at[i], d2l.at[t, ds], a2_send.at[1, t, ds], d2_recv.at[1, t, ds], device(d, 0, core)) for t, d in ((0, 1), (1, back))]

    def send_near(i, t, ds):
        d = (1, back)[t]
        return [remote(obuf.at[i], aro.at[t, ds], a_send.at[0, t, ds], ar_recv.at[0, t, ds], device(d, 0, core)),
                remote(lbuf.at[i], arl.at[t, ds], a_send.at[1, t, ds], ar_recv.at[1, t, ds], device(d, 0, core))]

    def add_far(i, t, ds):
        for c in send_far(i, ds)[t::2]:
            c.wait_recv()
        for u in range(pair):
            h = t * pair + u
            o, lse = merge([(obuf[i, h], lbuf[i, h:h + 1, :]), (d2o[t, ds, u], d2l[t, ds, h:h + 1, :])])
            obuf[i, h] = o.astype(jnp.bfloat16)
            lbuf[i, h:h + 1, :] = lse

    def send_home(ds):
        if ds == 2:
            return [c for t, d in ((0, 1), (1, back)) for c in (
                remote(bo.at[ds, t], bfo.at[t], b_send.at[0, t, ds], bf_recv.at[0, t], device(0, d, core)),
                remote(bl.at[ds, t], bfl.at[t], b_send.at[1, t, ds], bf_recv.at[1, t], device(0, d, core)))]
        return [c for t in (0, 1) for c in (
            remote(bo.at[ds, t], fo.at[core, ds], b_send.at[0, t, ds], b_recv.at[0, core, ds], device(0, ds, t)),
            remote(bl.at[ds, t], fl.at[core, ds], b_send.at[1, t, ds], b_recv.at[1, core, ds], device(0, ds, t)))]

    def gather_row(i, ds):
        for t in (0, 1):
            for c in send_near(i, t, ds):
                c.wait_recv()
        far = {1: 0, back: 1}.get(ds)
        if far is not None:
            for c in send_home(2)[2 * far:2 * far + 2]:
                c.wait_recv()
        for h in range(heads):
            for t in (0, 1):
                at = slice(t * half_cols, (t + 1) * half_cols)
                parts = [(obuf[i, h, :, at], lbuf[i, h:h + 1, at])] + [(aro[d, ds, h, :, at], arl[d, ds, h:h + 1, at]) for d in (0, 1)]
                if t == far:
                    parts.append((bfo[t, h], bfl[t, h:h + 1, :]))
                o, lse = merge(parts)
                bo[ds, t, h] = o.astype(jnp.bfloat16)
                bl[ds, t, h:h + 1, :] = lse

    slot_run(-1, ())
    local_q.wait()
    for d in swaps:
        d.wait_recv()

    for h in range(heads):
        kcat[h] = jnp.concatenate([kx[core, h], kx[2, h]], axis=0)
        vcat[h] = jnp.concatenate([vx[core, h], vx[2, h]], axis=0).astype(jnp.float32).T.astype(jnp.bfloat16)

    col = lax.broadcasted_iota(jnp.int32, (1, cols), 1)
    q_toks = {}
    for late in set(lead):
        row = col - jnp.where(col >= half_cols, half_cols, 0) - late
        for g in range(ratio):
            row = row - jnp.where(row >= tok, tok, 0)
        q_toks[late] = row + jnp.where(col >= half_cols, tok, 0)

    def digit(axis, i):
        low, high = (sum(order[first + k][axis] * side ** k for k in range(8)) for first in (0, 8))
        k = i % 8
        power = (1 + (side - 1) * (k % 2)) * (1 + (side ** 2 - 1) * ((k // 2) % 2)) * (1 + (side ** 4 - 1) * (k // 4))
        return ((low + (high - low) * (i // 8)) // power) % side

    def place(i):
        return digit(0, i), digit(1, i)

    bufs = (s0, s1)
    tiles = [(n, a) for n in (0, 1) for a in range(0, cache_len, QK_CHUNK)]

    def scores(i, h, s_ref, found):
        df, ds = place(i)
        where = slot(df, ds)
        at = h * n_rows - lead[h]
        q = jnp.concatenate([qbuf[where, j, at:at + half_cols] for j in (0, 1)], axis=0)
        m8 = jnp.full((8, cols), MASK_FILL, jnp.float32)
        for n, a in tiles + [(2, 0)]:
            k = kcat[h] if n == 2 else kbuf[(core, 2)[n], h, a:a + QK_CHUNK, :]
            sc = lax.dot_general(k, q, (((1,), (1,)), ((), ())), preferred_element_type=jnp.float32)
            for r in range(0, k.shape[0], ROW_STEP):
                t = sc[r:r + ROW_STEP] * scale
                if n < 2:
                    bias = bias_ref[n, a + r:a + r + ROW_STEP, :]
                    t = t + jnp.concatenate([bias, bias], axis=1)
                else:
                    step = lax.broadcasted_iota(jnp.int32, t.shape, 0) + r % n_new
                    first_key = (2 * chip + (core, other)[r // n_new]) * tok - 2 * where * tok
                    t = jnp.where((first_key + step <= q_toks[lead[h]]) & (step < tok), t, MASK_FILL)
                at = n * cache_len + a + r
                s_ref[at:at + ROW_STEP, :] = t
                for u in range(0, ROW_STEP, 8):
                    m8 = jnp.maximum(m8, t[u:u + 8])
                yield
        found.append(jnp.max(m8, axis=0, keepdims=True))

    def values(i, h, s_ref, m):
        l8 = jnp.zeros((8, cols), jnp.float32)
        acc = None
        for n, a in [(n, a) for n in (0, 1) for a in range(0, cache_len, PV_CHUNK)] + [(2, 0)]:
            v = vcat[h] if n == 2 else vbuf[(core, 2)[n], h, :, a:a + PV_CHUNK]
            ps = []
            for r in range(0, v.shape[1], ROW_STEP):
                at = n * cache_len + a + r
                p = jnp.exp2(s_ref[at:at + ROW_STEP, :] - m)
                for u in range(0, ROW_STEP, 8):
                    l8 = l8 + p[u:u + 8]
                ps.append(p.astype(jnp.bfloat16))
                yield
            d = lax.dot_general(v, jnp.concatenate(ps, axis=0), (((1,), (0,)), ((), ())), preferred_element_type=jnp.float32)
            acc = d if acc is None else acc + d
        l = jnp.sum(l8, axis=0, keepdims=True)
        obuf[i, h] = (acc * (1.0 / l)).astype(jnp.bfloat16)
        lbuf[i, h:h + 1, :] = m + jnp.log2(l)
        yield

    def run(*gens):
        live = list(gens)
        while live:
            for g in list(live):
                try:
                    next(g)
                except StopIteration:
                    live.remove(g)

    for j in (0, 1):
        want(*order[0], j)
    found = []
    run(scores(0, 0, s0, found))

    def body(i, m):
        nxt = i + 1 - (i + 1) // n_blocks
        for h in range(heads):
            if h * SLOTS % heads == 0:
                at = h * SLOTS // heads
                for part in range(0, n_blocks, side):
                    def some(part=part):
                        for k in range(part, part + side):
                            if (k, at) in works:
                                pl.when(i == k)(works[k, at])
                    pl.when(i // side == part // side)(some)
            found = []
            last = h + 1 == heads
            run(values(i, h, bufs[h % 2], m), scores(nxt if last else i, 0 if last else h + 1, bufs[(h + 1) % 2], found))
            m = found[0]
        return m

    works = {}
    for n in range(n_blocks * SLOTS):
        fresh = []
        if n % SLOTS == SLOTS - 1 and n // SLOTS + 1 < n_blocks:
            fresh += [(*order[n // SLOTS + 1], j) for j in (0, 1)]
        fresh += [q_piece(code) for code in PLAN.get(n, ()) if code < 10000]
        fresh = [w for w in dict.fromkeys(fresh) if w not in seen]
        seen.update(fresh)
        if fresh or n in PLAN:
            works[divmod(n, SLOTS)] = functools.partial(slot_run, n, fresh)

    lax.fori_loop(0, n_blocks, body, found[0])
    slot_run(n_blocks * SLOTS, ())
    gather_row(order.index((0, 0)), 0)
    to_sibling = [remote(bo.at[0, other], fo.at[core, 0], b_send.at[0, 0, 0], b_recv.at[0, core, 0], device(0, 0, other)),
                  remote(bl.at[0, other], fl.at[core, 0], b_send.at[1, 0, 0], b_recv.at[1, core, 0], device(0, 0, other))]
    for c in to_sibling:
        c.start()
    fo[core, 0] = bo[0, core]
    fl[core, 0] = bl[0, core]

    near = (0, 1, back)
    for ds in near[1:]:
        for k in (0, 1):
            remote(bo.at[ds, k], fo.at[k, ds], b_send.at[0, 0, 0], b_recv.at[0, k, ds], device(0, 0, core)).wait_recv()
            remote(bl.at[ds, k], fl.at[k, ds], b_send.at[0, 0, 0], b_recv.at[1, k, ds], device(0, 0, core)).wait_recv()
    remote(bo.at[0, 0], fo.at[other, 0], b_send.at[0, 0, 0], b_recv.at[0, other, 0], device(0, 0, core)).wait_recv()
    remote(bl.at[0, 0], fl.at[other, 0], b_send.at[0, 0, 0], b_recv.at[1, other, 0], device(0, 0, core)).wait_recv()
    for k in (0, 1):
        for h in range(heads):
            o, lse = merge([(fo[k, d, h], fl[k, d, h:h + 1, :]) for d in near])
            o = o.T
            for g in range(ratio):
                ostage[pl.ds((k * heads + h) * ratio + g, tok, stride=kv_heads * ratio), :] = o[lead[h] + g * tok:lead[h] + (g + 1) * tok]
            lstage[k * heads + h:k * heads + h + 1, :] = (pltpu.roll(lse, half_cols - lead[h], 1) if lead[h] else lse) * LN2
    out_ref[...] = ostage[...].astype(jnp.bfloat16)
    lse = lstage[:kv_heads, :]
    for g in range(ratio):
        lstage[pl.ds(kv_heads + g, kv_heads, stride=ratio), :] = lse if g == 0 else pltpu.roll(lse, half_cols - g * tok, 1)
    lse_ref[...] = lstage[kv_heads:kv_heads * (ratio + 1), :].T[:tok]

    for c in swaps + to_sibling + [swap_q] + [remote(qbuf.at[mine, 0], qbuf.at[mine, 0], sq.at[n], rq.at[mine, 0], device(0, 0, core)) for n in sends]:
        c.wait_send()
    for ds in range(side):
        for c in send_far(0, ds) + send_near(0, 0, ds) + send_near(0, 1, ds):
            c.wait_send()
    for ds in range(1, side):
        for c in send_home(ds):
            c.wait_send()


def solution(mesh):
    groups = mesh.shape['cp']
    side = math.isqrt(groups // 2)
    tok_spec = P(('dp', 'cp'))

    def local_attend(queries, key_new, value_new, key_cache, value_cache, prefix_len):
        tok, heads, dim = queries.shape
        cache_len, kv_heads = key_cache.shape[:2]
        ratio = heads // kv_heads
        half = kv_heads // 2
        rows = tok * ratio
        rows_pad = rows + -rows % 128
        new_pad = -tok % 16
        n_new = tok + new_pad
        keys = 2 * (cache_len + n_new)
        chunk = cache_len // 4
        n_blocks = side * side
        bf, f32 = jnp.bfloat16, jnp.float32
        cols = 2 * rows_pad
        dma = pltpu.SemaphoreType.DMA
        out, lse = pl.pallas_call(
            functools.partial(attend, side, tok, ratio, cache_len),
            in_specs=[pl.BlockSpec(memory_space=pltpu.SMEM)] + [pl.BlockSpec(memory_space=pltpu.HBM)] * 5,
            out_specs=[pl.BlockSpec(memory_space=pltpu.VMEM)] * 2,
            out_shape=[jax.ShapeDtypeStruct((tok * heads, dim), bf), jax.ShapeDtypeStruct((tok, heads), f32)],
            scratch_shapes=[
                pltpu.VMEM((tok * heads, dim), bf), pltpu.VMEM((tok * kv_heads, dim), bf), pltpu.VMEM((tok * kv_heads, dim), bf),
                pltpu.VMEM((cache_len * kv_heads, dim), bf), pltpu.VMEM((cache_len * kv_heads, dim), bf),
                pltpu.VMEM((2, chunk * kv_heads, dim), f32), pltpu.VMEM((2, half * rows, dim), bf),
                pltpu.VMEM((tok * heads, dim), f32), pltpu.VMEM((kv_heads * (ratio + 1), rows_pad), f32),
                pltpu.VMEM((2, cache_len, 128), f32),
                pltpu.VMEM((keys, cols), f32), pltpu.VMEM((keys, cols), f32),
                pltpu.VMEM((n_blocks, 2, half * rows, dim), bf),
                pltpu.VMEM((3, half, cache_len, dim), bf), pltpu.VMEM((3, half, dim, cache_len), bf),
                pltpu.VMEM((3, half, n_new, dim), bf), pltpu.VMEM((3, half, n_new, dim), bf),
                pltpu.VMEM((half, 2 * n_new, dim), bf), pltpu.VMEM((half, dim, 2 * n_new), bf),
                pltpu.VMEM((n_blocks, half, dim, cols), bf), pltpu.VMEM((n_blocks, half, cols), f32),
                pltpu.VMEM((2, side, half // 2, dim, cols), bf), pltpu.VMEM((2, side, half, cols), f32),
                pltpu.VMEM((2, side, half, dim, cols), bf), pltpu.VMEM((2, side, half, cols), f32),
                pltpu.VMEM((side, 2, half, dim, rows_pad), bf), pltpu.VMEM((side, 2, half, rows_pad), f32),
                pltpu.VMEM((2, side, half, dim, rows_pad), bf), pltpu.VMEM((2, side, half, rows_pad), f32),
                dma((5, 4)), dma((n_blocks, 2)), dma((40,)), dma((3,)), dma((2, 5)), dma((2, 5)), dma,
                dma((2, 2, side)), dma((2, 2, side)), dma((2, 2, side)), dma((2, 2, side)), dma((2, 2, side)), dma((2, 2, side)), dma((2, 2)),
                pltpu.VMEM((2, half, dim, rows_pad), bf), pltpu.VMEM((2, half, rows_pad), f32),
            ],
            compiler_params=pltpu.CompilerParams(collective_id=0, has_side_effects=True, vmem_limit_bytes=52 * 1024 * 1024),
            name='attend',
        )(prefix_len, *[a.reshape(-1, dim) for a in (queries, key_new, value_new, key_cache, value_cache)])
        return out.reshape(tok, heads, dim), lse

    return jax.shard_map(local_attend, mesh=mesh, in_specs=(tok_spec, tok_spec, tok_spec, tok_spec, tok_spec, P('dp')), out_specs=(tok_spec, tok_spec), check_vma=False)
```
